512 devices in a mesh: gx: 8 (over y_hi, x), gy: 4 (over y_lo, core), gz: 16 (over z).
Axes of the slice: x: 4, y: 4 (y_hi: 2, y_lo: 2; y = y_hi * 2 + y_lo), z: 16, core: 2. Of those that a mesh axis runs over, the one named last changes fastest.
Arguments:
- fields: float32 [6, 128, 64, 2048], P(None, 'gx', 'gy', 'gz'), may hold values from -6 to 6
- permittivity: float32 [128, 64, 2048], P('gx', 'gy', 'gz'), may hold values from 1 to 4
- donor_owner: int32 [65536, 1], P(('gx', 'gy', 'gz')), may hold values from 0 to 63; in each aligned block of 128 rows (0 to 127, 128 to 255, ...) at most 4 rows name the same one
- donor_base: int32 [65536, 3], P(('gx', 'gy', 'gz')), may hold values from 0 to 127, as said below
- donor_weights: float32 [65536, 15], P(('gx', 'gy', 'gz')), may hold values from -3 to 3
Outputs:
- new_fields: float32 [6, 128, 64, 2048], P(None, 'gx', 'gy', 'gz')
- receptor_values: float32 [6, 65536], P(None, ('gx', 'gy', 'gz'))
The draws below stay inside these ranges and needn't reach their ends.
Inputs may be any that keep to these rules, and one draw needn't show every extreme that they name: `donor_owner`: within the 128 rows of one device no owner index is named by more than 4 rows, and one is named by exactly 4. `donor_base`: column 0 lies in 0 to 15, column 1 in 0 to 15, column 2 in 0 to 127.
All inputs are finite; a program needn't handle non-finite values.
Results may differ from the reference program's by a relative error of at most 0.00002.
Values sent between devices are 32-bit elements; how exact they have to be, the bound alone decides.
No kernel may reach another device: no remote copies, remote signals or barrier semaphores. Data moves between devices by JAX's collectives and lax.ppermute only.
A program may use at most 192 MiB of HBM per device.

```python
import math
import jax
import jax.numpy as jnp
import numpy as np
from jax import lax

CX = 16
CY = 16
CZ = 128
R_DEV = 128
CAP = 4
NX = 128
NY = 64
NZ = 2048
RECEPT = 65536
N_GY = 4
N_GZ = 16
DEVICES = 512


def draw_donor_base(key, part):
    first = jax.random.randint(jax.random.fold_in(key, 11), (RECEPT, 1), 0, CX, dtype=jnp.int32)
    second = jax.random.randint(jax.random.fold_in(key, 12), (RECEPT, 1), 0, CY, dtype=jnp.int32)
    third = jax.random.randint(jax.random.fold_in(key, 13), (RECEPT, 1), 0, CZ, dtype=jnp.int32)
    return jnp.concatenate([first, second, third], 1)


def steps_of(rng, extent, pieces, low, largest):
    gain, own = 1.0, jax.random.fold_in(rng, 6)
    for position, blocks in pieces:
        heights = jnp.exp(jax.random.uniform(jax.random.fold_in(own, position), (blocks,), jnp.float32, low / len(pieces), largest / len(pieces)))
        gain = gain * jnp.repeat(heights, extent[position] // blocks).reshape([-1 if axis == position else 1 for axis in range(len(extent))])
    return gain


def shared_out(stream_key, own, number, rows, amount, top, most, lean):
    sequence = jax.random.permutation(stream_key, amount)
    packed, common = shares(amount, rows * top, most, lean, True), shares(amount, rows * top, most, lean, False)
    places = jnp.arange(amount)

    def named(tallies, offset_by):
        used = int((tallies > 0).sum())
        fixed = max(1, used // 4)
        passed = fixed + (places - fixed + offset_by * (used - fixed)) % max(1, amount - fixed)
        return jnp.zeros((amount,), jnp.int32).at[sequence[jnp.where(places < fixed, places, passed)]].set(jnp.asarray(tallies, jnp.int32))

    tallies = jnp.where(number % 4 == 0, named(packed, number // 4), named(common, number - number // 4 - 1))
    mixed = jax.random.permutation(jax.random.fold_in(own, 3), amount)
    source_of, sink = mixed[0:amount // 2 * 2:2], mixed[1:amount // 2 * 2:2]
    room = jnp.minimum(tallies[source_of] - 1, most - tallies[sink]) // 2
    room = jnp.where((source_of == sequence[0]) | (sink == sequence[0]) | (tallies[sink] == 0), 0, jnp.maximum(room, 0))
    passed = jax.random.randint(jax.random.fold_in(own, 4), (amount // 2,), 0, 1 << 20) % (room + 1)
    tallies = tallies.at[source_of].add(-passed).at[sink].add(passed)
    labels = jnp.searchsorted(jnp.cumsum(tallies), jnp.arange(rows * top), side="right").astype(jnp.int32)
    grid = labels.reshape(top, rows).T
    grid = grid[jax.random.permutation(jax.random.fold_in(own, 1), rows)]
    offset_by = jax.random.randint(jax.random.fold_in(own, 2), (rows, 1), 0, top)
    return jnp.take_along_axis(grid, (jnp.arange(top)[None, :] + offset_by) % top, axis=1)


def shares(number_of, total, limit, slope, full):
    portions = [(1 << 20) // math.isqrt(standing ** slope) + 1 for standing in range(1, number_of + 1)]
    largest = limit if full else min(limit, max(-(-total // number_of), total * portions[0] // sum(portions)))
    least = 1 if total - largest >= number_of - 1 else 0
    holding, spare = [largest] + [least] * (number_of - 1), total - largest - least * (number_of - 1)
    while spare > 0:
        movable = [i for i in range(1, number_of) if holding[i] < largest] or [i for i in range(1, number_of) if holding[i] < limit]
        whole, budget = sum([portions[i] for i in movable]), spare
        for i in movable:
            addition = min(limit - holding[i], max(1, budget * portions[i] // whole), spare)
            holding[i] = holding[i] + addition
            spare = spare - addition
    return np.array(holding)


def bell_draw(own_key, shape, scale, most, cuts=(), kind=jnp.bfloat16):
    loudness = steps_of(own_key, shape, cuts, -0.22, 0.18) if cuts else 1.0
    values = jax.random.normal(own_key, shape, jnp.float32) * scale * loudness
    return jnp.minimum(jnp.maximum(values, -most), most).astype(kind)


def setup_inputs(seed: int = 0) -> dict:
    streams_of = jax.random.split(jax.random.key(seed), 6)
    fields = bell_draw(streams_of[0], (6, NX, NY, NZ), 1.0, 6.0, ((1, 8), (2, 4), (3, 16)), jnp.float32)
    permittivity = jnp.clip(jnp.exp(math.log(4.0) - 1.3862944 * jax.random.uniform(streams_of[1], (NX, NY, NZ), jnp.float32) ** steps_of(streams_of[1], (NX, NY, NZ), ((0, 8), (1, 4), (2, 16)), -0.2, 0.2)), 1.0, 4.0)
    donor_owner_keys = jax.random.split(jax.random.fold_in(streams_of[2], 1), RECEPT // R_DEV)
    donor_owner_turns = jax.random.permutation(jax.random.fold_in(streams_of[2], 3), RECEPT // R_DEV)
    donor_owner = jax.vmap(lambda own, number: shared_out(jax.random.fold_in(streams_of[2], 2), own, number, R_DEV, N_GY * N_GZ, 1, CAP, 2))(donor_owner_keys, donor_owner_turns).reshape((RECEPT, 1))
    donor_base = draw_donor_base(jax.random.fold_in(streams_of[5], 71), 0)
    donor_weights = bell_draw(streams_of[4], (RECEPT, 15), 0.5, 3.0, ((0, 512),), jnp.float32)
    return {"fields": fields, "permittivity": permittivity, "donor_owner": donor_owner, "donor_base": donor_base, "donor_weights": donor_weights}


step_size = 0.25


def shifted(field, axis_index, offset):
    window = [slice(2, -2), slice(2, -2), slice(2, -2)]
    length = field.shape[axis_index] - 4
    window[axis_index] = slice(2 + offset, 2 + offset + length)
    return field[tuple(window)]


def derivative(field, axis_index):
    outer = shifted(field, axis_index, -2) - shifted(field, axis_index, 2)
    inner = shifted(field, axis_index, 1) - shifted(field, axis_index, -1)
    return (outer + 8.0 * inner) / 12.0


def curl_rate(padded, coefficient):
    rate_ex = (derivative(padded[5], 1) - derivative(padded[4], 2)) / coefficient
    rate_ey = (derivative(padded[3], 2) - derivative(padded[5], 0)) / coefficient
    rate_ez = (derivative(padded[4], 0) - derivative(padded[3], 1)) / coefficient
    rate_hx = derivative(padded[1], 2) - derivative(padded[2], 1)
    rate_hy = derivative(padded[2], 0) - derivative(padded[0], 2)
    rate_hz = derivative(padded[0], 1) - derivative(padded[1], 0)
    return jnp.stack([rate_ex, rate_ey, rate_ez, rate_hx, rate_hy, rate_hz])


def contract(donor_tiles, weights):
    weight_x = weights[0:5]
    weight_y = weights[5:10]
    weight_z = weights[10:15]
    along_z = jnp.sum(donor_tiles * weight_z[None, None, None, :, :], axis=3)
    along_y = jnp.sum(along_z * weight_y[None, None, :, :], axis=2)
    return jnp.sum(along_y * weight_x[None, :, :], axis=1)


def reference(fields, permittivity, donor_owner, donor_base, donor_weights):
    accumulated = fields
    taylor_term = fields
    for power in range(1, 5):
        padded = jnp.pad(taylor_term, ((0, 0), (2, 2), (2, 2), (2, 2)))
        taylor_term = (step_size / power) * curl_rate(padded, permittivity)
        accumulated = accumulated + taylor_term
    new_fields = accumulated
    donor_grid = jnp.pad(new_fields, ((0, 0), (2, 2), (2, 2), (2, 2)))
    group_size = N_GY * N_GZ
    device_id = jnp.arange(RECEPT, dtype=jnp.int32) // R_DEV
    plane_id = device_id // group_size
    owner_id = donor_owner[:, 0].astype(jnp.int32)
    row_x = plane_id * CX + donor_base[:, 0]
    row_y = (owner_id // N_GZ) * CY + donor_base[:, 1]
    row_z = (owner_id % N_GZ) * CZ + donor_base[:, 2]
    corners = jnp.stack([row_x, row_y, row_z], 1).astype(jnp.int32).reshape(DEVICES, R_DEV, 3)
    weights = donor_weights.reshape(DEVICES, R_DEV, 15)

    def one_block(block_item):
        corner_rows, weight_rows = block_item
        donor_tiles = jax.vmap(
            lambda corner: lax.dynamic_slice(donor_grid, (jnp.int32(0), corner[0], corner[1], corner[2]), (6, 5, 5, 5)),
            out_axes=4)(corner_rows)
        return contract(donor_tiles, weight_rows.T)

    values = lax.map(one_block, (corners, weights))
    receptor_values = jnp.transpose(values, (1, 0, 2)).reshape(6, RECEPT)
    return new_fields, receptor_values
```

```python
import jax
import jax.numpy as jnp
from jax import lax
from jax.experimental import pallas as pl
from jax.experimental.pallas import tpu as pltpu
from jax.sharding import PartitionSpec as P

STEP = 0.25
CX, CY, CZ = 16, 16, 128
GX, GZ = 10, 10
NF = 7
PAIRS = NF * CX
ZPER, YPER = 12, 6
ZGROUPS = -(-PAIRS // ZPER)
YGROUPS = -(-PAIRS // YPER)
XW = CX + 2 * GX
STRIDE = 20
EXACT = lax.Precision.HIGHEST
F32 = jnp.float32


def x_list():
    entries = []
    for k in range(1, 5):
        entries += [(k, c, t) for c in range(NF) for t in (0, 1, 2, 3)]
    for k in range(5, 9):
        entries += [(k, c, t) for c in range(NF) for t in (1, 2, 4)]
    for k in range(9, 11):
        entries += [(k, c, t) for c in (1, 2, 4, 5) for t in (1, 2)]
    return entries


XLIST = x_list()
XROWS = len(XLIST)
XGROUPS = -(-XROWS // YPER)


def roll(value, shift, axis):
    size = value.shape[axis]
    shift = shift % size
    return value if shift == 0 else pltpu.roll(value, shift, axis)


def lanes(shape):
    return lax.broadcasted_iota(jnp.int32, shape, len(shape) - 1)


def rows_of(shape):
    return lax.broadcasted_iota(jnp.int32, shape, len(shape) - 2)


def vmem(count):
    return [pl.BlockSpec(memory_space=pltpu.VMEM)] * count


def call(body, outs, ins, limit, scratch=(), flops=1000000):
    many = isinstance(outs, list)
    return pl.pallas_call(
        body,
        out_shape=[jax.ShapeDtypeStruct(s, F32) for s in outs] if many else jax.ShapeDtypeStruct(outs, F32),
        in_specs=vmem(len(ins)),
        out_specs=vmem(len(outs)) if many else vmem(1)[0],
        scratch_shapes=list(scratch),
        compiler_params=pltpu.CompilerParams(vmem_limit_bytes=limit * 1048576),
        cost_estimate=pl.CostEstimate(flops=flops, bytes_accessed=1000000, transcendentals=0),
    )(*ins)


def pack_z(f_ref, e_ref, lo_ref, hi_ref, inv_ref):
    inv_ref[...] = 1.0 / e_ref[...]
    lane = lanes((CY, CZ))
    for g in range(ZGROUPS):
        lo = jnp.zeros((CY, CZ), F32)
        hi = jnp.zeros((CY, CZ), F32)
        for j in range(min(ZPER, PAIRS - g * ZPER)):
            c, x = divmod(g * ZPER + j, CX)
            tile = f_ref[c, x] if c < 6 else inv_ref[x]
            lo = lo + roll(jnp.where(lane < GZ, tile, 0.0), GZ * j, 1)
            hi = hi + roll(jnp.where(lane >= CZ - GZ, tile, 0.0), GZ * (j + 1), 1)
        lo_ref[g] = lo
        hi_ref[g] = hi


def pack_y(f_ref, inv_ref, zlo_ref, zhi_ref, h_ref, lo_ref, hi_ref):
    lane = lanes((CY, CZ))
    for g in range(YGROUPS):
        lo = jnp.zeros((8, CZ), F32)
        hi = jnp.zeros((8, CZ), F32)
        for j in range(min(YPER, PAIRS - g * YPER)):
            p = g * YPER + j
            c, x = divmod(p, CX)
            zg, zj = divmod(p, ZPER)
            below = roll(zlo_ref[zg], CZ - GZ - GZ * zj, 1)
            above = roll(zhi_ref[zg], -GZ * zj, 1)
            ghost = jnp.where(lane >= CZ - GZ, below, jnp.where(lane < GZ, above, 0.0))
            h_ref[c, x] = ghost
            tile = f_ref[c, x] if c < 6 else inv_ref[x]
            lo_ref[p] = tile[0:8]
            hi_ref[p] = tile[8:16]
            packed = roll(ghost, GZ + 2 * GZ * j, 1)
            lo = lo + packed[0:8]
            hi = hi + packed[8:16]
        lo_ref[PAIRS + g] = lo
        hi_ref[PAIRS + g] = hi


def ring_lanes(packed, j, lane):
    moved = roll(packed, -(GZ + 2 * GZ * j), 1)
    return jnp.where((lane < GZ) | (lane >= CZ - GZ), moved, 0.0)


def pack_x(f_ref, inv_ref, h_ref, ylo_ref, yhi_ref, lo_ref, hi_ref):
    lane = lanes((8, CZ))
    row = rows_of((8, CZ))

    def tile_of(c, x, t):
        p = c * CX + x
        if t in (1, 2):
            own = pl.ds(8 * (t - 1), 8)
            main = f_ref[c, x, own] if c < 6 else inv_ref[x, own]
            return main, h_ref[c, x, own]
        if t == 4:
            a, b = tile_of(c, x, 0), tile_of(c, x, 3)
            return jnp.where(row >= 4, a[0], b[0]), jnp.where(row >= 4, a[1], b[1])
        ref = ylo_ref if t == 0 else yhi_ref
        return ref[p], ring_lanes(ref[PAIRS + p // YPER], p % YPER, lane)

    for ref, side in ((lo_ref, 0), (hi_ref, 1)):
        for g in range(XGROUPS):
            total = jnp.zeros((8, CZ), F32)
            for j in range(min(YPER, XROWS - g * YPER)):
                n = g * YPER + j
                k, c, t = XLIST[n]
                main, ghost = tile_of(c, k - 1 if side == 0 else CX - k, t)
                ref[n] = main
                total = total + roll(ghost, GZ + 2 * GZ * j, 1)
            ref[XROWS + g] = total


def along_y(tiles, t, row):
    before, here, after = tiles[(t - 1) % 4], tiles[t], tiles[(t + 1) % 4]
    down = lambda d: roll(jnp.where(row >= 8 - d, before, here), d, 0)
    up = lambda d: roll(jnp.where(row < d, after, here), -d, 0)
    return up(1) - down(1), down(2) - up(2)


def along_z(here, other, lane):
    down = lambda d: roll(jnp.where(lane >= CZ - d, other, here), d, 1)
    up = lambda d: roll(jnp.where(lane < d, other, here), -d, 1)
    return up(1) - down(1), down(2) - up(2)


def taylor(source, inv_ref, x, tiles, scale, put):
    row = rows_of((8, CZ))
    lane = lanes((8, CZ))
    for t in tiles:
        for half in (0, 1):
            def dx(c):
                at = lambda d: source[half, c, x + d, t]
                return at(1) - at(-1), at(-2) - at(2)

            def dy(c):
                near = {u % 4: source[half, c, x, u % 4] for u in (t - 1, t, t + 1)}
                return along_y(near, t, row)

            def dz(c):
                return along_z(source[half, c, x, t], source[1 - half, c, x, t], lane)

            def rate(plus, minus):
                return (plus[1] - minus[1]) + 8.0 * (plus[0] - minus[0])

            inv = inv_ref[half, 6, x, t]
            electric = inv * scale
            magnetic = jnp.where(inv > 0.0, scale, 0.0)
            put(half, 0, t, electric * rate(dy(5), dz(4)))
            put(half, 1, t, electric * rate(dz(3), dx(5)))
            put(half, 2, t, electric * rate(dx(4), dy(3)))
            put(half, 3, t, magnetic * rate(dz(1), dy(2)))
            put(half, 4, t, magnetic * rate(dx(2), dz(0)))
            put(half, 5, t, magnetic * rate(dy(0), dx(1)))


def dot(a, b, da=1, db=0):
    return lax.dot_general(a, b, (((da,), (db,)), ((), ())), precision=EXACT, preferred_element_type=F32)


def spread(count, parity):
    shape = (count, 128)
    return (lanes(shape) == rows_of(shape) + parity * 64).astype(F32)


def compute(
    f_ref, own_inv_ref, h_ref, ylo_ref, yhi_ref, xlo_ref, xhi_ref, req_ref,
    new_ref, ans_ref,
    full, t1, t2, t3, acc, words, wz, wxy, spill, parts,
):
    lane = lanes((8, CZ))
    row = rows_of((8, CZ))
    zero = jnp.zeros((8, CZ), F32)
    for p in range(PAIRS):
        c, x = divmod(p, CX)
        for t in (1, 2):
            own = pl.ds(8 * (t - 1), 8)
            full[0, c, GX + x, t] = f_ref[c, x, own] if c < 6 else own_inv_ref[x, own]
            full[1, c, GX + x, t] = h_ref[c, x, own]
        for ref, t in ((ylo_ref, 0), (yhi_ref, 3)):
            full[0, c, GX + x, t] = ref[p]
            full[1, c, GX + x, t] = ring_lanes(ref[PAIRS + p // YPER], p % YPER, lane)
    for side in (0, 1):
        ref = xlo_ref if side == 0 else xhi_ref
        for n, (k, c, t) in enumerate(XLIST):
            x = GX - k if side == 0 else GX + CX + k - 1
            pair = (ref[n], ring_lanes(ref[XROWS + n // YPER], n % YPER, lane))
            for half in (0, 1):
                if t == 4:
                    full[half, c, x, 0] = jnp.where(row >= 4, pair[half], 0.0)
                    full[half, c, x, 3] = jnp.where(row >= 4, 0.0, pair[half])
                else:
                    full[half, c, x, t] = pair[half]
        for k in (9, 10):
            x = GX - k if side == 0 else GX + CX + k - 1
            for c in (1, 2, 4, 5):
                for half in (0, 1):
                    full[half, c, x, 0] = zero
                    full[half, c, x, 3] = zero

    for power, source, target in ((1, full, t1), (2, t1, t2), (3, t2, t3)):
        def body(x, carry, source=source, target=target, power=power):
            def put(half, c, t, value):
                target[half, c, x, t] = value

            taylor(source, full, x, (0, 1, 2, 3), STEP / power / 12.0, put)
            return carry

        lax.fori_loop(2 * power, XW - 2 * power, body, 0)

    def last(x, carry):
        def put(half, c, t, value):
            total = full[half, c, x, t] + t1[half, c, x, t]
            total = total + t2[half, c, x, t]
            total = total + t3[half, c, x, t]
            acc[half, c, x - 8, t - 1] = total + value

        taylor(t3, full, x, (1, 2), STEP / 4 / 12.0, put)
        return carry

    lax.fori_loop(8, XW - 8, last, 0)
    for c in range(6):
        for t in (0, 1):
            new_ref[c, :, pl.ds(8 * t, 8), :] = acc[0, c, 2:18, t]

    req = req_ref[...]
    words[0] = dot(req, spread(64, 0), 0, 0)
    words[1] = dot(req, spread(64, 1), 0, 0)

    def word(pair, w):
        even = words[0, pl.ds(2 * pair * STRIDE + w, 1), :]
        return even + words[1, pl.ds((2 * pair + 1) * STRIDE + w, 1), :]

    cell = rows_of((CZ, 128)).astype(F32)
    low = rows_of((8, 128)).astype(F32)
    for pair in range(6):
        kind, at = divmod(pair, 2)
        columns = pl.ds(128 * at, 128)
        bx, by, bz = word(pair, 0), word(pair, 1), word(pair, 2)
        wx = [word(pair, 3 + i) for i in range(5)]
        wy = [word(pair, 8 + i) for i in range(5)]
        wz_rows = [word(pair, 13 + i) for i in range(5)]

        def weights(position, base, values):
            away = position - base
            total = jnp.zeros(away.shape, F32)
            for i in range(5):
                total = jnp.where(away == float(i), values[i], total)
            return total

        wz[kind, pl.ds(0, CZ), columns] = weights(cell + 2.0, bz, wz_rows)
        wz[kind, pl.ds(CZ, CZ), columns] = jnp.zeros((CZ, 128), F32)
        wz[kind, pl.ds(CZ, 8), columns] = weights(low + (CZ + 2.0), bz, wz_rows)
        wz[kind, pl.ds(2 * CZ - 8, 8), columns] = weights(low - 6.0, bz, wz_rows)
        in_x = [weights(jnp.full((1, 128), float(x), F32), bx, wx) for x in range(CX + 4)]
        for t in (0, 1):
            in_y = weights(low + (8.0 * t + 2.0), by, wy)
            for x in range(CX + 4):
                if kind == 0:
                    wxy[x, t, :, columns] = in_x[x] * in_y
                elif kind == 2 - t:
                    spill[kind - 1, x, :, columns] = in_x[x] * in_y

    parts[...] = jnp.zeros((48, 128), F32)
    for c in range(6):
        def both(t):
            grid = [acc[half, c] if t is None else acc[half, c, :, t] for half in (0, 1)]
            return jnp.concatenate([g.reshape(-1, CZ) for g in grid], axis=1)

        for kind, t, weight in ((0, None, wxy), (1, 1, spill.at[0]), (2, 0, spill.at[1])):
            along = dot(both(t), wz[kind])
            product = along * weight[...].reshape(along.shape)
            total = jnp.sum(product, axis=0, keepdims=True)
            for at in (0, 1):
                parts[pl.ds((2 * kind + at) * 8 + c, 1), :] = total[:, 128 * at:128 * at + 128]
    values = parts[...]
    blank = jnp.zeros((16, 128), F32)
    filled = jnp.concatenate([values, blank], axis=0)
    empty = jnp.zeros((64, 128), F32)
    ans_ref[...] = dot(spread(64, 0), jnp.concatenate([filled, empty], axis=0), 1, 1) + dot(
        spread(64, 1), jnp.concatenate([empty, filled], axis=0), 1, 1
    )


def requests(data_ref, send_ref, pick_ref, rank_ref):
    data = data_ref[...]
    wide = (128, 128)
    owner = jnp.broadcast_to(data[:, 18:19], wide)
    base_y = jnp.broadcast_to(data[:, 1:2], wide)
    r, q = rows_of(wide), lanes(wide)
    owner_row = jnp.sum(jnp.where(r == q, owner, 0.0), axis=0, keepdims=True)
    base_row = jnp.sum(jnp.where(r == q, base_y, 0.0), axis=0, keepdims=True)
    same = owner == owner_row
    rank_col = jnp.sum(jnp.where(same & (q < r), 1.0, 0.0), axis=1, keepdims=True)
    rank_row = jnp.sum(jnp.where(same & (r < q), 1.0, 0.0), axis=0, keepdims=True)
    rank_ref[...] = jnp.broadcast_to(rank_row, (8, 128))

    lane = lanes((128, 256))
    slot, w = lane // STRIDE, lane % STRIDE
    word_row = rows_of((128, 256))
    copies = jnp.where((lanes((128, 256)) % STRIDE == word_row) & (word_row < 18) & (lane < 12 * STRIDE), 1.0, 0.0)
    spread_out = dot(data, copies)
    moved = jnp.where(w == 1, jnp.where(slot // 4 == 1, float(CY), jnp.where(slot // 4 == 2, -float(CY), 0.0)), 0.0)
    chosen = (slot % 4).astype(F32) == rank_col
    spread_out = jnp.where(chosen, spread_out + moved, 0.0)

    place = rows_of((64, 128)).astype(F32)
    total = jnp.zeros((64, 256), F32)
    for kind, move in ((0, 0.0), (1, -16.0), (2, 16.0)):
        hit = place == owner_row + move
        if kind == 1:
            hit = hit & (base_row < 2.0)
        if kind == 2:
            hit = hit & (base_row > 13.0)
        pick = jnp.where(hit, 1.0, 0.0)
        pick_ref[kind] = pick
        total = total + dot(pick, jnp.where(slot // 4 == kind, spread_out, 0.0))
    send_ref[...] = total


def collect(ans_ref, pick_ref, rank_ref, out_ref):
    ans = ans_ref[...]
    rank = rank_ref[...]
    total = jnp.zeros((8, 128), F32)
    for kind in range(3):
        got = dot(ans, pick_ref[kind], 0, 0)
        for j in range(4):
            start = (j % 2) * 64 + (2 * kind + j // 2) * 8
            total = total + jnp.where(rank == float(j), got[start:start + 8], 0.0)
    out_ref[...] = total[0:6]


def shift_both(low_edge, high_edge, axis):
    size = lax.axis_size(axis)
    up = [(i, i + 1) for i in range(size - 1)]
    down = [(i + 1, i) for i in range(size - 1)]
    return lax.ppermute(high_edge, axis, up), lax.ppermute(low_edge, axis, down)


def local(fields, permittivity, donor_owner, donor_base, donor_weights):
    data = jnp.concatenate(
        [
            donor_base.astype(F32),
            donor_weights,
            donor_owner.astype(F32),
            jnp.zeros((donor_owner.shape[0], 128 - 19), F32),
        ],
        axis=1,
    )
    zshape = (ZGROUPS, CY, CZ)
    zlo, zhi, inv = call(pack_z, [zshape, zshape, (CX, CY, CZ)], (fields, permittivity), 16)
    zlo, zhi = shift_both(zlo, zhi, "gz")
    yshape = (PAIRS + YGROUPS, 8, CZ)
    ghosts, ylo, yhi = call(pack_y, [(NF, CX, CY, CZ), yshape, yshape], (fields, inv, zlo, zhi), 16)
    ylo, yhi = shift_both(ylo, yhi, "gy")
    xshape = (XROWS + XGROUPS, 8, CZ)
    xlo, xhi = call(pack_x, [xshape, xshape], (fields, inv, ghosts, ylo, yhi), 20)
    send, pick, rank = call(requests, [(64, 256), (3, 64, 128), (8, 128)], (data,), 8)
    send, xlo, xhi = lax.optimization_barrier((send, xlo, xhi))
    xlo, xhi = shift_both(xlo, xhi, "gx")
    req = lax.all_to_all(send, ("gy", "gz"), 0, 0, tiled=True)
    big = pltpu.VMEM((2, 6, XW, 4, 8, CZ), F32)
    new_fields, answers = call(
        compute,
        [(6, CX, CY, CZ), (64, 128)],
        (fields, inv, ghosts, ylo, yhi, xlo, xhi, req),
        48,
        scratch=[
            pltpu.VMEM((2, NF, XW, 4, 8, CZ), F32),
            big,
            big,
            big,
            pltpu.VMEM((2, 6, CX + 4, 2, 8, CZ), F32),
            pltpu.VMEM((2, 256, 128), F32),
            pltpu.VMEM((3, 256, 256), F32),
            pltpu.VMEM((CX + 4, 2, 8, 256), F32),
            pltpu.VMEM((2, CX + 4, 8, 256), F32),
            pltpu.VMEM((48, 128), F32),
        ],
        flops=100000000,
    )
    answers = lax.all_to_all(answers, ("gy", "gz"), 0, 0, tiled=True)
    receptor_values = call(collect, (6, 128), (answers, pick, rank), 8)
    return new_fields, receptor_values


def solution(mesh):
    placed = (
        P(None, "gx", "gy", "gz"),
        P("gx", "gy", "gz"),
        P(("gx", "gy", "gz"), None),
        P(("gx", "gy", "gz"), None),
        P(("gx", "gy", "gz"), None),
    )
    return jax.shard_map(
        local,
        mesh=mesh,
        in_specs=placed,
        out_specs=(P(None, "gx", "gy", "gz"), P(None, ("gx", "gy", "gz"))),
        check_vma=False,
    )
```

```python
import jax
import jax.numpy as jnp
from jax import lax
from jax.experimental import pallas as pl
from jax.experimental.pallas import tpu as pltpu
from jax.sharding import PartitionSpec as P

STEP = 0.25
CX, CY, CZ = 16, 16, 128
GX, GZ = 10, 10
NF = 7
PAIRS = NF * CX
ZGROUPS = CX // 2 + 2
XW = CX + 2 * GX
STRIDE = 20
EXACT = lax.Precision.HIGHEST
F32 = jnp.float32


def z_slot(c, x):
    return (x // 2, (x % 2) * 6 + c) if c < 6 else (CX // 2 + x // 8, x % 8)


def x_lists():
    main = []
    for k in range(1, 5):
        main += [(k, c, t) for c in range(NF) for t in (0, 1, 2, 3)]
    for k in range(5, 7):
        main += [(k, c, t) for c in range(NF) for t in (1, 2, 4)]
    for k in range(7, 9):
        main += [(k, c, t) for c in range(NF) for t in (1, 2)]
        main += [(k, c, 4) for c in (0, 3)]
    for k in range(9, 11):
        main += [(k, c, t) for c in (1, 2, 4, 5) for t in (1, 2)]
    ends = []
    for q in range(5):
        ends += [(q, t, e) for t in ((0, 1, 2, 3), (0, 1, 2, 3), (1, 2, 4), (1, 2, 4), (1, 2))[q] for e in (0, 1)]
    ends += [(5, t, e) for t in (0, 1, 2, 3) for e in (0, 1)]
    return main, ends


XMAIN, XENDS = x_lists()
XROWS = len(XMAIN)
XEND = {key: XROWS + n for n, key in enumerate(XENDS)}
XTOTAL = XROWS + len(XENDS)
YTOTAL = PAIRS + 2 * ZGROUPS


def roll(value, shift, axis):
    size = value.shape[axis]
    shift = shift % size
    return value if shift == 0 else pltpu.roll(value, shift, axis)


def lanes(shape):
    return lax.broadcasted_iota(jnp.int32, shape, len(shape) - 1)


def rows_of(shape):
    return lax.broadcasted_iota(jnp.int32, shape, len(shape) - 2)


def vmem(count):
    return [pl.BlockSpec(memory_space=pltpu.VMEM)] * count


def call(body, outs, ins, limit, scratch=(), flops=1000000):
    many = isinstance(outs, list)
    return pl.pallas_call(
        body,
        out_shape=[jax.ShapeDtypeStruct(s, F32) for s in outs] if many else jax.ShapeDtypeStruct(outs, F32),
        in_specs=vmem(len(ins)),
        out_specs=vmem(len(outs)) if many else vmem(1)[0],
        scratch_shapes=list(scratch),
        compiler_params=pltpu.CompilerParams(vmem_limit_bytes=limit * 1048576),
        cost_estimate=pl.CostEstimate(flops=flops, bytes_accessed=1000000, transcendentals=0),
    )(*ins)


def pack_z(f_ref, e_ref, lo_ref, hi_ref, inv_ref):
    inv_ref[...] = 1.0 / e_ref[...]
    lane = lanes((CY, CZ))
    sums = {}
    for x in range(CX):
        for c in range(NF):
            g, s = z_slot(c, x)
            tile = f_ref[c, x] if c < 6 else inv_ref[x]
            for side, keep in ((0, lane < GZ), (1, lane >= CZ - GZ)):
                part = roll(jnp.where(keep, tile, 0.0), GZ * (s + 1), 1)
                sums[g, side] = sums[g, side] + part if (g, side) in sums else part
    for g in range(ZGROUPS):
        lo_ref[g] = sums[g, 0]
        hi_ref[g] = sums[g, 1]


def pack_y(f_ref, inv_ref, zlo_ref, zhi_ref, lo_ref, hi_ref):
    for out, start in ((lo_ref, 0), (hi_ref, 8)):
        rows = pl.ds(start, 8)
        for p in range(PAIRS):
            c, x = divmod(p, CX)
            out[p] = f_ref[c, x, rows] if c < 6 else inv_ref[x, rows]
        for g in range(ZGROUPS):
            out[PAIRS + g] = zlo_ref[g, rows]
            out[PAIRS + ZGROUPS + g] = zhi_ref[g, rows]


def z_ends(lo, hi, s, lane):
    first = lane < GZ * (s + 1) if s < 11 else (lane >= GZ * s) & (lane < GZ * (s + 1))
    moved = roll(jnp.where(first, lo, hi), CZ - GZ - GZ * s, 1)
    return jnp.where((lane < GZ) | (lane >= CZ - GZ), moved, 0.0)


def pack_x(f_ref, inv_ref, zlo_ref, zhi_ref, ylo_ref, yhi_ref, lo_ref, hi_ref):
    row = rows_of((8, CZ))

    def main_of(c, x, t):
        if t == 4:
            return jnp.where(row >= 4, main_of(c, x, 0), main_of(c, x, 3))
        if t in (1, 2):
            rows = pl.ds(8 * (t - 1), 8)
            return f_ref[c, x, rows] if c < 6 else inv_ref[x, rows]
        return (ylo_ref if t == 0 else yhi_ref)[c * CX + x]

    def end_of(g, t, e):
        if t == 4:
            return jnp.where(row >= 4, end_of(g, 0, e), end_of(g, 3, e))
        if t in (1, 2):
            return (zhi_ref if e else zlo_ref)[g, pl.ds(8 * (t - 1), 8)]
        return (ylo_ref if t == 0 else yhi_ref)[PAIRS + e * ZGROUPS + g]

    for out, side in ((lo_ref, 0), (hi_ref, 1)):
        for n, (k, c, t) in enumerate(XMAIN):
            out[n] = main_of(c, CX - k if side else k - 1, t)
        for (q, t, e), n in XEND.items():
            g = CX // 2 + side if q == 5 else (CX // 2 - 1 - q if side else q)
            out[n] = end_of(g, t, e)


def along_y(tiles, t, row):
    before, here, after = tiles[(t - 1) % 4], tiles[t], tiles[(t + 1) % 4]
    down = lambda d: roll(jnp.where(row >= 8 - d, before, here), d, 0)
    up = lambda d: roll(jnp.where(row < d, after, here), -d, 0)
    return up(1) - down(1), down(2) - up(2)


def along_z(here, other, lane):
    down = lambda d: roll(jnp.where(lane >= CZ - d, other, here), d, 1)
    up = lambda d: roll(jnp.where(lane < d, other, here), -d, 1)
    return up(1) - down(1), down(2) - up(2)


def taylor(source, inv_ref, x, tiles, scale, put, comps=(0, 1, 2, 3, 4, 5)):
    row = rows_of((8, CZ))
    lane = lanes((8, CZ))
    for t in tiles:
        for half in (0, 1):
            def dx(c):
                at = lambda d: source[half, c, x + d, t]
                return at(1) - at(-1), at(-2) - at(2)

            def dy(c):
                near = {u % 4: source[half, c, x, u % 4] for u in (t - 1, t, t + 1)}
                return along_y(near, t, row)

            def dz(c):
                return along_z(source[half, c, x, t], source[1 - half, c, x, t], lane)

            rates = (
                lambda: (dy(5), dz(4)),
                lambda: (dz(3), dx(5)),
                lambda: (dx(4), dy(3)),
                lambda: (dz(1), dy(2)),
                lambda: (dx(2), dz(0)),
                lambda: (dy(0), dx(1)),
            )
            inv = inv_ref[half, 6, x, t]
            electric = inv * scale
            magnetic = jnp.where(inv > 0.0, scale, 0.0)
            for c in comps:
                plus, minus = rates[c]()
                rate = (plus[1] - minus[1]) + 8.0 * (plus[0] - minus[0])
                put(half, c, t, (electric if c < 3 else magnetic) * rate)


def dot(a, b, da=1, db=0):
    return lax.dot_general(a, b, (((da,), (db,)), ((), ())), precision=EXACT, preferred_element_type=F32)


def spread(count, parity):
    shape = (count, 128)
    return (lanes(shape) == rows_of(shape) + parity * 64).astype(F32)


def compute(
    f_ref, own_inv_ref, zlo_ref, zhi_ref, ylo_ref, yhi_ref, xlo_ref, xhi_ref, req_ref,
    new_ref, ans_ref,
    full, t1, t2, t3, acc, words, wz, wxy, spill, parts,
):
    lane = lanes((8, CZ))
    row = rows_of((8, CZ))
    zero = jnp.zeros((8, CZ), F32)
    for p in range(PAIRS):
        c, x = divmod(p, CX)
        g, s = z_slot(c, x)
        for t in (1, 2):
            own = pl.ds(8 * (t - 1), 8)
            full[0, c, GX + x, t] = f_ref[c, x, own] if c < 6 else own_inv_ref[x, own]
            full[1, c, GX + x, t] = z_ends(zlo_ref[g, own], zhi_ref[g, own], s, lane)
        for ref, t in ((ylo_ref, 0), (yhi_ref, 3)):
            full[0, c, GX + x, t] = ref[p]
            full[1, c, GX + x, t] = z_ends(ref[PAIRS + g], ref[PAIRS + ZGROUPS + g], s, lane)
    for side in (0, 1):
        ref = xhi_ref if side == 0 else xlo_ref
        where_main = {key: n for n, key in enumerate(XMAIN)}
        for k in range(1, GX + 1):
            x = GX + CX + k - 1 if side == 0 else GX - k
            for c in range(NF):
                if k > 8 and c in (0, 3, 6):
                    continue
                g, s = z_slot(c, k - 1 if side == 0 else CX - k)
                q = 5 if c == 6 else (k - 1) // 2
                done = set()
                for t in (0, 1, 2, 3, 4):
                    pair = [None, None]
                    if (k, c, t) in where_main:
                        pair[0] = ref[where_main[k, c, t]]
                    if (q, t, 0) in XEND:
                        pair[1] = z_ends(ref[XEND[q, t, 0]], ref[XEND[q, t, 1]], s, lane)
                    for half in (0, 1):
                        if pair[half] is None:
                            continue
                        if t == 4:
                            full[half, c, x, 0] = jnp.where(row >= 4, pair[half], 0.0)
                            full[half, c, x, 3] = jnp.where(row >= 4, 0.0, pair[half])
                            done |= {(half, 0), (half, 3)}
                        else:
                            full[half, c, x, t] = pair[half]
                            done.add((half, t))
                for half in (0, 1):
                    for t in (0, 3):
                        if (half, t) not in done:
                            full[half, c, x, t] = zero

    for power, source, target in ((1, full, t1), (2, t1, t2), (3, t2, t3)):
        scale = STEP / power / 12.0

        def body(x, carry, source=source, target=target, scale=scale):
            def put(half, c, t, value):
                target[half, c, x, t] = value

            taylor(source, full, x, (0, 1, 2, 3), scale, put)
            return carry

        def edge(i, carry, source=source, target=target, scale=scale, power=power):
            x = jnp.where(i < 2, 2 * power + i, XW - 2 * power - 4 + i)

            def put(half, c, t, value):
                target[half, c, x, t] = value

            taylor(source, full, x, (1, 2), scale, put, (1, 2, 4, 5))
            return carry

        lax.fori_loop(0, 4, edge, 0, unroll=2)
        lax.fori_loop(2 * power + 2, XW - 2 * power - 2, body, 0, unroll=2)

    def last(x, carry):
        def put(half, c, t, value):
            total = full[half, c, x, t] + t1[half, c, x, t]
            total = total + t2[half, c, x, t]
            total = total + t3[half, c, x, t]
            acc[half, c, x - 8, t - 1] = total + value

        taylor(t3, full, x, (1, 2), STEP / 4 / 12.0, put)
        return carry

    lax.fori_loop(8, XW - 8, last, 0, unroll=2)
    for c in range(6):
        for t in (0, 1):
            new_ref[c, :, pl.ds(8 * t, 8), :] = acc[0, c, 2:18, t]

    req = req_ref[...]
    words[0] = dot(req, spread(64, 0), 0, 0)
    words[1] = dot(req, spread(64, 1), 0, 0)

    def word(pair, w):
        even = words[0, pl.ds(2 * pair * STRIDE + w, 1), :]
        return even + words[1, pl.ds((2 * pair + 1) * STRIDE + w, 1), :]

    cell = rows_of((CZ, 128)).astype(F32)
    low = rows_of((8, 128)).astype(F32)
    for pair in range(6):
        kind, at = divmod(pair, 2)
        columns = pl.ds(128 * at, 128)
        bx, by, bz = word(pair, 0), word(pair, 1), word(pair, 2)
        wx = [word(pair, 3 + i) for i in range(5)]
        wy = [word(pair, 8 + i) for i in range(5)]
        wz_rows = [word(pair, 13 + i) for i in range(5)]

        def weights(position, base, values):
            away = position - base
            total = jnp.zeros(away.shape, F32)
            for i in range(5):
                total = jnp.where(away == float(i), values[i], total)
            return total

        wz[kind, pl.ds(0, CZ), columns] = weights(cell + 2.0, bz, wz_rows)
        wz[kind, pl.ds(CZ, CZ), columns] = jnp.zeros((CZ, 128), F32)
        wz[kind, pl.ds(CZ, 8), columns] = weights(low + (CZ + 2.0), bz, wz_rows)
        wz[kind, pl.ds(2 * CZ - 8, 8), columns] = weights(low - 6.0, bz, wz_rows)
        in_x = [weights(jnp.full((1, 128), float(x), F32), bx, wx) for x in range(CX + 4)]
        for t in (0, 1):
            in_y = weights(low + (8.0 * t + 2.0), by, wy)
            for x in range(CX + 4):
                if kind == 0:
                    wxy[x, t, :, columns] = in_x[x] * in_y
                elif kind == 2 - t:
                    spill[kind - 1, x, :, columns] = in_x[x] * in_y

    parts[...] = jnp.zeros((48, 128), F32)
    for c in range(6):
        def both(t):
            grid = [acc[half, c] if t is None else acc[half, c, :, t] for half in (0, 1)]
            return jnp.concatenate([g.reshape(-1, CZ) for g in grid], axis=1)

        for kind, t, weight in ((0, None, wxy), (1, 1, spill.at[0]), (2, 0, spill.at[1])):
            along = dot(both(t), wz[kind])
            product = along * weight[...].reshape(along.shape)
            total = jnp.sum(product, axis=0, keepdims=True)
            for at in (0, 1):
                parts[pl.ds((2 * kind + at) * 8 + c, 1), :] = total[:, 128 * at:128 * at + 128]
    values = parts[...]
    blank = jnp.zeros((16, 128), F32)
    filled = jnp.concatenate([values, blank], axis=0)
    empty = jnp.zeros((64, 128), F32)
    ans_ref[...] = dot(spread(64, 0), jnp.concatenate([filled, empty], axis=0), 1, 1) + dot(
        spread(64, 1), jnp.concatenate([empty, filled], axis=0), 1, 1
    )


def requests(data_ref, send_ref, pick_ref, rank_ref):
    data = data_ref[...]
    wide = (128, 128)
    owner = jnp.broadcast_to(data[:, 18:19], wide)
    base_y = jnp.broadcast_to(data[:, 1:2], wide)
    r, q = rows_of(wide), lanes(wide)
    owner_row = jnp.sum(jnp.where(r == q, owner, 0.0), axis=0, keepdims=True)
    base_row = jnp.sum(jnp.where(r == q, base_y, 0.0), axis=0, keepdims=True)
    same = owner == owner_row
    rank_col = jnp.sum(jnp.where(same & (q < r), 1.0, 0.0), axis=1, keepdims=True)
    rank_row = jnp.sum(jnp.where(same & (r < q), 1.0, 0.0), axis=0, keepdims=True)
    rank_ref[...] = jnp.broadcast_to(rank_row, (8, 128))

    lane = lanes((128, 256))
    slot, w = lane // STRIDE, lane % STRIDE
    word_row = rows_of((128, 256))
    copies = jnp.where((lanes((128, 256)) % STRIDE == word_row) & (word_row < 18) & (lane < 12 * STRIDE), 1.0, 0.0)
    spread_out = dot(data, copies)
    moved = jnp.where(w == 1, jnp.where(slot // 4 == 1, float(CY), jnp.where(slot // 4 == 2, -float(CY), 0.0)), 0.0)
    chosen = (slot % 4).astype(F32) == rank_col
    spread_out = jnp.where(chosen, spread_out + moved, 0.0)

    place = rows_of((64, 128)).astype(F32)
    total = jnp.zeros((64, 256), F32)
    for kind, move in ((0, 0.0), (1, -16.0), (2, 16.0)):
        hit = place == owner_row + move
        if kind == 1:
            hit = hit & (base_row < 2.0)
        if kind == 2:
            hit = hit & (base_row > 13.0)
        pick = jnp.where(hit, 1.0, 0.0)
        pick_ref[kind] = pick
        total = total + dot(pick, jnp.where(slot // 4 == kind, spread_out, 0.0))
    send_ref[...] = total


def collect(ans_ref, pick_ref, rank_ref, out_ref):
    ans = ans_ref[...]
    rank = rank_ref[...]
    total = jnp.zeros((8, 128), F32)
    for kind in range(3):
        got = dot(ans, pick_ref[kind], 0, 0)
        for j in range(4):
            start = (j % 2) * 64 + (2 * kind + j // 2) * 8
            total = total + jnp.where(rank == float(j), got[start:start + 8], 0.0)
    out_ref[...] = total[0:6]


def shift_both(low_edge, high_edge, axis):
    size = lax.axis_size(axis)
    up = [(i, i + 1) for i in range(size - 1)]
    down = [(i + 1, i) for i in range(size - 1)]
    return lax.ppermute(high_edge, axis, up), lax.ppermute(low_edge, axis, down)


def local(fields, permittivity, donor_owner, donor_base, donor_weights):
    data = jnp.concatenate(
        [
            donor_base.astype(F32),
            donor_weights,
            donor_owner.astype(F32),
            jnp.zeros((donor_owner.shape[0], 128 - 19), F32),
        ],
        axis=1,
    )
    zshape = (ZGROUPS, CY, CZ)
    zlo, zhi, inv = call(pack_z, [zshape, zshape, (CX, CY, CZ)], (fields, permittivity), 16)
    zlo, zhi = shift_both(zlo, zhi, "gz")
    yshape = (YTOTAL, 8, CZ)
    ylo, yhi = call(pack_y, [yshape, yshape], (fields, inv, zlo, zhi), 8)
    ylo, yhi = shift_both(ylo, yhi, "gy")
    xshape = (XTOTAL, 8, CZ)
    xlo, xhi = call(pack_x, [xshape, xshape], (fields, inv, zlo, zhi, ylo, yhi), 8)
    send, pick, rank = call(requests, [(64, 256), (3, 64, 128), (8, 128)], (data,), 8)
    send, xlo, xhi = lax.optimization_barrier((send, xlo, xhi))
    xlo, xhi = shift_both(xlo, xhi, "gx")
    req = lax.all_to_all(send, ("gy", "gz"), 0, 0, tiled=True)
    big = pltpu.VMEM((2, 6, XW, 4, 8, CZ), F32)
    new_fields, answers = call(
        compute,
        [(6, CX, CY, CZ), (64, 128)],
        (fields, inv, zlo, zhi, ylo, yhi, xlo, xhi, req),
        42,
        scratch=[
            pltpu.VMEM((2, NF, XW, 4, 8, CZ), F32),
            big,
            big,
            big,
            pltpu.VMEM((2, 6, CX + 4, 2, 8, CZ), F32),
            pltpu.VMEM((2, 256, 128), F32),
            pltpu.VMEM((3, 256, 256), F32),
            pltpu.VMEM((CX + 4, 2, 8, 256), F32),
            pltpu.VMEM((2, CX + 4, 8, 256), F32),
            pltpu.VMEM((48, 128), F32),
        ],
        flops=100000000,
    )
    answers = lax.all_to_all(answers, ("gy", "gz"), 0, 0, tiled=True)
    receptor_values = call(collect, (6, 128), (answers, pick, rank), 8)
    return new_fields, receptor_values


def solution(mesh):
    placed = (
        P(None, "gx", "gy", "gz"),
        P("gx", "gy", "gz"),
        P(("gx", "gy", "gz"), None),
        P(("gx", "gy", "gz"), None),
        P(("gx", "gy", "gz"), None),
    )
    return jax.shard_map(
        local,
        mesh=mesh,
        in_specs=placed,
        out_specs=(P(None, "gx", "gy", "gz"), P(None, ("gx", "gy", "gz"))),
        check_vma=False,
    )
```

```python
import jax
import jax.numpy as jnp
from jax import lax
from jax.experimental import pallas as pl
from jax.experimental.pallas import tpu as pltpu
from jax.sharding import PartitionSpec as P

STEP = 0.25
CX, CY, CZ = 16, 16, 128
GX, GZ = 10, 10
NF = 7
PAIRS = NF * CX
ZGROUPS = CX // 2 + 2
XW = CX + 2 * GX
STRIDE = 20
EXACT = lax.Precision.HIGHEST
F32 = jnp.float32


def z_slot(c, x):
    return (x // 2, (x % 2) * 6 + c) if c < 6 else (CX // 2 + x // 8, x % 8)


def x_lists():
    main = []
    for k in range(1, 5):
        main += [(k, c, t) for c in range(NF) for t in (0, 1, 2, 3)]
    for k in range(5, 7):
        main += [(k, c, t) for c in range(NF) for t in (1, 2, 4)]
    for k in range(7, 9):
        main += [(k, c, t) for c in range(NF) for t in (1, 2)]
        main += [(k, c, 4) for c in (0, 3)]
    for k in range(9, 11):
        main += [(k, c, t) for c in (1, 2, 4, 5) for t in (1, 2)]
    ends = []
    for q in range(5):
        ends += [(q, t, e) for t in ((0, 1, 2, 3), (0, 1, 2, 3), (1, 2, 4), (1, 2, 4), (1, 2))[q] for e in (0, 1)]
    ends += [(5, t, e) for t in (0, 1, 2, 3) for e in (0, 1)]
    return main, ends


XMAIN, XENDS = x_lists()
XROWS = len(XMAIN)
XEND = {key: XROWS + n for n, key in enumerate(XENDS)}
XTOTAL = XROWS + len(XENDS)
YTOTAL = PAIRS + 2 * ZGROUPS


def roll(value, shift, axis):
    size = value.shape[axis]
    shift = shift % size
    return value if shift == 0 else pltpu.roll(value, shift, axis)


def lanes(shape):
    return lax.broadcasted_iota(jnp.int32, shape, len(shape) - 1)


def rows_of(shape):
    return lax.broadcasted_iota(jnp.int32, shape, len(shape) - 2)


def vmem(count):
    return [pl.BlockSpec(memory_space=pltpu.VMEM)] * count


def call(body, outs, ins, limit, scratch=(), flops=1000000, space=pltpu.VMEM):
    many = isinstance(outs, list)
    return pl.pallas_call(
        body,
        out_shape=[jax.ShapeDtypeStruct(s, F32) for s in outs] if many else jax.ShapeDtypeStruct(outs, F32),
        in_specs=[pl.BlockSpec(memory_space=space)] * len(ins),
        out_specs=vmem(len(outs)) if many else vmem(1)[0],
        scratch_shapes=list(scratch),
        compiler_params=pltpu.CompilerParams(vmem_limit_bytes=limit * 1048576),
        cost_estimate=pl.CostEstimate(flops=flops, bytes_accessed=1000000, transcendentals=0),
    )(*ins)


def pack_z(f_hbm, e_hbm, lo_ref, hi_ref, inv_ref, f_ref, e_ref, sems):
    copies = [pltpu.make_async_copy(e_hbm, e_ref, sems.at[0])]
    for g in range(4):
        part = pl.ds(4 * g, 4)
        copies.append(pltpu.make_async_copy(f_hbm.at[:, part], f_ref.at[:, part], sems.at[g + 1]))
    for copy in copies:
        copy.start()
    lane = lanes((CY, CZ))
    sums = {}

    def add(c, x, tile):
        g, s = z_slot(c, x)
        for side, keep in ((0, lane < GZ), (1, lane >= CZ - GZ)):
            part = roll(jnp.where(keep, tile, 0.0), GZ * (s + 1), 1)
            sums[g, side] = sums[g, side] + part if (g, side) in sums else part

    copies[0].wait()
    inv_ref[...] = 1.0 / e_ref[...]
    for x in range(CX):
        add(6, x, inv_ref[x])
    for g in range(4):
        copies[g + 1].wait()
        for x in range(4 * g, 4 * g + 4):
            for c in range(6):
                add(c, x, f_ref[c, x])
    for g in range(ZGROUPS):
        lo_ref[g] = sums[g, 0]
        hi_ref[g] = sums[g, 1]


def pack_y(f_ref, inv_ref, zlo_ref, zhi_ref, lo_ref, hi_ref):
    for out, start in ((lo_ref, 0), (hi_ref, 8)):
        rows = pl.ds(start, 8)
        for p in range(PAIRS):
            c, x = divmod(p, CX)
            out[p] = f_ref[c, x, rows] if c < 6 else inv_ref[x, rows]
        for g in range(ZGROUPS):
            out[PAIRS + g] = zlo_ref[g, rows]
            out[PAIRS + ZGROUPS + g] = zhi_ref[g, rows]


def z_ends(lo, hi, s, lane):
    first = lane < GZ * (s + 1) if s < 11 else (lane >= GZ * s) & (lane < GZ * (s + 1))
    moved = roll(jnp.where(first, lo, hi), CZ - GZ - GZ * s, 1)
    return jnp.where((lane < GZ) | (lane >= CZ - GZ), moved, 0.0)


def pack_x(f_ref, inv_ref, zlo_ref, zhi_ref, ylo_ref, yhi_ref, lo_ref, hi_ref):
    row = rows_of((8, CZ))

    def main_of(c, x, t):
        if t == 4:
            return jnp.where(row >= 4, main_of(c, x, 0), main_of(c, x, 3))
        if t in (1, 2):
            rows = pl.ds(8 * (t - 1), 8)
            return f_ref[c, x, rows] if c < 6 else inv_ref[x, rows]
        return (ylo_ref if t == 0 else yhi_ref)[c * CX + x]

    def end_of(g, t, e):
        if t == 4:
            return jnp.where(row >= 4, end_of(g, 0, e), end_of(g, 3, e))
        if t in (1, 2):
            return (zhi_ref if e else zlo_ref)[g, pl.ds(8 * (t - 1), 8)]
        return (ylo_ref if t == 0 else yhi_ref)[PAIRS + e * ZGROUPS + g]

    for out, side in ((lo_ref, 0), (hi_ref, 1)):
        for n, (k, c, t) in enumerate(XMAIN):
            out[n] = main_of(c, CX - k if side else k - 1, t)
        for (q, t, e), n in XEND.items():
            g = CX // 2 + side if q == 5 else (CX // 2 - 1 - q if side else q)
            out[n] = end_of(g, t, e)


def taylor(source, inv_ref, band, x, tiles, scale, put, comps=(0, 1, 2, 3, 4, 5)):
    row = rows_of((8, CZ))
    def load(half, c, t, d=0):
        return source[half, c, x + d, t % 4]

    def dx(c):
        return {
            (half, t): (
                load(half, c, t, 1) - load(half, c, t, -1),
                load(half, c, t, 2) - load(half, c, t, -2),
            )
            for half in (0, 1)
            for t in tiles
        }

    def dy(c):
        out = {}
        for half in (0, 1):
            u = {}
            for t in sorted({v % 4 for t in tiles for v in (t, t + 1)}):
                here = load(half, c, t)
                u[t] = here - roll(jnp.where(row >= 6, load(half, c, t - 1), here), 2, 0)
            for t in tiles:
                low, high = u[t], u[(t + 1) % 4]
                near = roll(jnp.where(row < 1, high, low), -1, 0)
                out[half, t] = (near, roll(jnp.where(row < 2, high, low), -2, 0) + low)
        return out

    def all_dz(fields):
        block = jnp.concatenate(
            [jnp.concatenate([load(0, c, t), load(1, c, t)], axis=1) for c in fields for t in tiles], axis=0
        )
        high = block.astype(jnp.bfloat16)
        rest = block - high.astype(F32)
        middle = rest.astype(jnp.bfloat16)
        low = (rest - middle.astype(F32)).astype(jnp.bfloat16)
        total = sum(
            jnp.dot(part, band[...], preferred_element_type=F32) for part in (low, middle, high)
        )
        out = {}
        for i, c in enumerate(fields):
            for j, t in enumerate(tiles):
                start = 8 * (i * len(tiles) + j)
                for half in (0, 1):
                    out[c, half, t] = total[start:start + 8, 128 * half:128 * half + 128]
        return out

    pairs = ((dy, 5, 4, 0), (None, 3, 5, dx), (dx, 4, 3, dy), (None, 1, 2, dy), (dx, 2, 0, 0), (dy, 0, 1, dx))
    along_z = all_dz([c for c in (4, 3, 1, 0) if {4: 0, 3: 1, 1: 3, 0: 4}[c] in comps])
    factors = {}
    for half in (0, 1):
        for t in tiles:
            inv = inv_ref[half, 6, x, t]
            factors[half, t] = (inv * scale, jnp.where(inv > 0.0, scale, 0.0))
    for c in comps:
        first, c1, c2, second = pairs[c]
        plus = first(c1) if first else None
        minus = second(c2) if second else None
        for key in factors:
            if plus and minus:
                rate = 8.0 * (plus[key][0] - minus[key][0]) - (plus[key][1] - minus[key][1])
            elif plus:
                rate = 8.0 * plus[key][0] - plus[key][1] - along_z[(c2,) + key]
            else:
                rate = along_z[(c1,) + key] - (8.0 * minus[key][0] - minus[key][1])
            put(key[0], c, key[1], factors[key][c // 3] * rate)


def dot(a, b, da=1, db=0):
    return lax.dot_general(a, b, (((da,), (db,)), ((), ())), precision=EXACT, preferred_element_type=F32)


def spread(count, parity):
    shape = (count, 128)
    return (lanes(shape) == rows_of(shape) + parity * 64).astype(F32)


def compute(
    f_ref, own_inv_ref, zlo_ref, zhi_ref, ylo_ref, yhi_ref, xlo_ref, xhi_ref, req_ref,
    new_ref, ans_ref,
    full, t1, t2, t3, acc, words, wz, wxy, spill, edge_rows, parts, band,
):
    lane = lanes((8, CZ))
    row = rows_of((8, CZ))
    zero = jnp.zeros((8, CZ), F32)
    for p in range(PAIRS):
        c, x = divmod(p, CX)
        g, s = z_slot(c, x)
        for t in (1, 2):
            own = pl.ds(8 * (t - 1), 8)
            full[0, c, GX + x, t] = f_ref[c, x, own] if c < 6 else own_inv_ref[x, own]
            full[1, c, GX + x, t] = z_ends(zlo_ref[g, own], zhi_ref[g, own], s, lane)
        for ref, t in ((ylo_ref, 0), (yhi_ref, 3)):
            full[0, c, GX + x, t] = ref[p]
            full[1, c, GX + x, t] = z_ends(ref[PAIRS + g], ref[PAIRS + ZGROUPS + g], s, lane)
    for side in (0, 1):
        ref = xhi_ref if side == 0 else xlo_ref
        where_main = {key: n for n, key in enumerate(XMAIN)}
        for k in range(1, GX + 1):
            x = GX + CX + k - 1 if side == 0 else GX - k
            for c in range(NF):
                if k > 8 and c in (0, 3, 6):
                    continue
                g, s = z_slot(c, k - 1 if side == 0 else CX - k)
                q = 5 if c == 6 else (k - 1) // 2
                done = set()
                for t in (0, 1, 2, 3, 4):
                    pair = [None, None]
                    if (k, c, t) in where_main:
                        pair[0] = ref[where_main[k, c, t]]
                    if (q, t, 0) in XEND:
                        pair[1] = z_ends(ref[XEND[q, t, 0]], ref[XEND[q, t, 1]], s, lane)
                    for half in (0, 1):
                        if pair[half] is None:
                            continue
                        if t == 4:
                            full[half, c, x, 0] = jnp.where(row >= 4, pair[half], 0.0)
                            full[half, c, x, 3] = jnp.where(row >= 4, 0.0, pair[half])
                            done |= {(half, 0), (half, 3)}
                        else:
                            full[half, c, x, t] = pair[half]
                            done.add((half, t))
                for half in (0, 1):
                    for t in (0, 3):
                        if (half, t) not in done:
                            full[half, c, x, t] = zero

    ring = (rows_of((256, 256)) - lanes((256, 256)) + 256) % 256
    one = lambda d: (ring == d % 256).astype(F32)
    band[...] = (8.0 * (one(1) - one(-1)) + one(-2) - one(2)).astype(jnp.bfloat16)

    for power, source, target in ((1, full, t1), (2, t1, t2), (3, t2, t3)):
        scale = STEP / power / 12.0

        def body(x, carry, source=source, target=target, scale=scale):
            def put(half, c, t, value):
                target[half, c, x, t] = value

            taylor(source, full, band, x, (0, 1, 2, 3), scale, put)
            return carry

        def edge(i, carry, source=source, target=target, scale=scale, power=power):
            x = jnp.where(i < 2, 2 * power + i, XW - 2 * power - 4 + i)

            def put(half, c, t, value):
                target[half, c, x, t] = value

            taylor(source, full, band, x, (1, 2), scale, put, (1, 2, 4, 5))
            return carry

        lax.fori_loop(0, 4, edge, 0, unroll=2)
        lax.fori_loop(2 * power + 2, XW - 2 * power - 2, body, 0, unroll=4)

    def last(x, carry):
        def put(half, c, t, value):
            total = full[half, c, x, t] + t1[half, c, x, t]
            total = total + t2[half, c, x, t]
            total = total + t3[half, c, x, t]
            acc[half, c, x - 8, t - 1] = total + value

        taylor(t3, full, band, x, (1, 2), STEP / 4 / 12.0, put)
        return carry

    lax.fori_loop(8, XW - 8, last, 0, unroll=4)
    for c in range(6):
        for t in (0, 1):
            new_ref[c, :, pl.ds(8 * t, 8), :] = acc[0, c, 2:18, t]

    req = req_ref[...]
    words[0] = dot(req, spread(64, 0), 0, 0)
    words[1] = dot(req, spread(64, 1), 0, 0)

    def word(pair, w):
        even = words[0, pl.ds(2 * pair * STRIDE + w, 1), :]
        return even + words[1, pl.ds((2 * pair + 1) * STRIDE + w, 1), :]

    cell = rows_of((CZ, 128)).astype(F32)
    low = rows_of((8, 128)).astype(F32)
    for pair in range(6):
        kind, at = divmod(pair, 2)
        columns = pl.ds(128 * at, 128)
        bx, by, bz = word(pair, 0), word(pair, 1), word(pair, 2)
        wx = [word(pair, 3 + i) for i in range(5)]
        wy = [word(pair, 8 + i) for i in range(5)]
        wz_rows = [word(pair, 13 + i) for i in range(5)]

        def weights(position, base, values):
            away = position - base
            total = jnp.zeros(away.shape, F32)
            for i in range(5):
                total = jnp.where(away == float(i), values[i], total)
            return total

        wz[kind, pl.ds(0, CZ), columns] = weights(cell + 2.0, bz, wz_rows)
        wz[kind, pl.ds(CZ, CZ), columns] = jnp.zeros((CZ, 128), F32)
        wz[kind, pl.ds(CZ, 8), columns] = weights(low + (CZ + 2.0), bz, wz_rows)
        wz[kind, pl.ds(2 * CZ - 8, 8), columns] = weights(low - 6.0, bz, wz_rows)
        in_x = [weights(jnp.full((1, 128), float(x), F32), bx, wx) for x in range(CX + 4)] if kind == 0 else []
        if kind == 0:
            for t in (0, 1):
                in_y = weights(low + (8.0 * t + 2.0), by, wy)
                for x in range(CX + 4):
                    wxy[x, t, :, columns] = in_x[x] * in_y
        else:
            pair_row = rows_of((8, 128))
            in_y = weights((pair_row % 2).astype(F32) + (16.0 if kind == 1 else 2.0), by, wy)
            for g in range(CX // 4 + 1):
                along = weights((pair_row // 2 + 4 * g).astype(F32), bx, wx)
                spill[kind - 1, g, :, columns] = along * in_y

    for kind in (0, 1):
        for half in (0, 1):
            for c in range(6):
                for g in range(CX // 4 + 1):
                    total = None
                    for i in range(4):
                        tile = acc[half, c, 4 * g + i, 1 - kind]
                        moved = roll(tile, 2 * i - (6 if kind == 0 else 0), 0)
                        total = moved if total is None else jnp.where(row >= 2 * i, moved, total)
                    edge_rows[kind, half, c, g] = total

    parts[...] = jnp.zeros((48, 128), F32)
    for kind in range(3):
        grid = [acc[half] if kind == 0 else edge_rows[kind - 1, half] for half in (0, 1)]
        weight = wxy[...].reshape(-1, 256) if kind == 0 else spill[kind - 1].reshape(-1, 256)
        along = dot(jnp.concatenate([g.reshape(-1, CZ) for g in grid], axis=1), wz[kind])
        count = weight.shape[0]
        for c in range(6):
            total = jnp.sum(along[c * count:c * count + count] * weight, axis=0, keepdims=True)
            for at in (0, 1):
                parts[pl.ds((2 * kind + at) * 8 + c, 1), :] = total[:, 128 * at:128 * at + 128]
    values = parts[...]
    blank = jnp.zeros((16, 128), F32)
    filled = jnp.concatenate([values, blank], axis=0)
    empty = jnp.zeros((64, 128), F32)
    ans_ref[...] = dot(spread(64, 0), jnp.concatenate([filled, empty], axis=0), 1, 1) + dot(
        spread(64, 1), jnp.concatenate([empty, filled], axis=0), 1, 1
    )


def requests(data_ref, send_ref, pick_ref, rank_ref):
    data = data_ref[...]
    wide = (128, 128)
    owner = jnp.broadcast_to(data[:, 18:19], wide)
    base_y = jnp.broadcast_to(data[:, 1:2], wide)
    r, q = rows_of(wide), lanes(wide)
    owner_row = jnp.sum(jnp.where(r == q, owner, 0.0), axis=0, keepdims=True)
    base_row = jnp.sum(jnp.where(r == q, base_y, 0.0), axis=0, keepdims=True)
    same = owner == owner_row
    rank_col = jnp.sum(jnp.where(same & (q < r), 1.0, 0.0), axis=1, keepdims=True)
    rank_row = jnp.sum(jnp.where(same & (r < q), 1.0, 0.0), axis=0, keepdims=True)
    rank_ref[...] = jnp.broadcast_to(rank_row, (8, 128))

    lane = lanes((128, 256))
    slot, w = lane // STRIDE, lane % STRIDE
    word_row = rows_of((128, 256))
    copies = jnp.where((lanes((128, 256)) % STRIDE == word_row) & (word_row < 18) & (lane < 12 * STRIDE), 1.0, 0.0)
    spread_out = dot(data, copies)
    moved = jnp.where(w == 1, jnp.where(slot // 4 == 1, float(CY), jnp.where(slot // 4 == 2, -float(CY), 0.0)), 0.0)
    chosen = (slot % 4).astype(F32) == rank_col
    spread_out = jnp.where(chosen, spread_out + moved, 0.0)

    place = rows_of((64, 128)).astype(F32)
    total = jnp.zeros((64, 256), F32)
    for kind, move in ((0, 0.0), (1, -16.0), (2, 16.0)):
        hit = place == owner_row + move
        if kind == 1:
            hit = hit & (base_row < 2.0)
        if kind == 2:
            hit = hit & (base_row > 13.0)
        pick = jnp.where(hit, 1.0, 0.0)
        pick_ref[kind] = pick
        total = total + dot(pick, jnp.where(slot // 4 == kind, spread_out, 0.0))
    send_ref[...] = total


def collect(ans_ref, pick_ref, rank_ref, out_ref):
    ans = ans_ref[...]
    rank = rank_ref[...]
    total = jnp.zeros((8, 128), F32)
    for kind in range(3):
        got = dot(ans, pick_ref[kind], 0, 0)
        for j in range(4):
            start = (j % 2) * 64 + (2 * kind + j // 2) * 8
            total = total + jnp.where(rank == float(j), got[start:start + 8], 0.0)
    out_ref[...] = total[0:6]


def shift_both(low_edge, high_edge, axis):
    size = lax.axis_size(axis)
    up = [(i, i + 1) for i in range(size - 1)]
    down = [(i + 1, i) for i in range(size - 1)]
    return lax.ppermute(high_edge, axis, up), lax.ppermute(low_edge, axis, down)


def local(fields, permittivity, donor_owner, donor_base, donor_weights):
    data = jnp.concatenate(
        [
            donor_base.astype(F32),
            donor_weights,
            donor_owner.astype(F32),
            jnp.zeros((donor_owner.shape[0], 128 - 19), F32),
        ],
        axis=1,
    )
    zshape = (ZGROUPS, CY, CZ)
    zlo, zhi, inv = call(
        pack_z,
        [zshape, zshape, (CX, CY, CZ)],
        (fields, permittivity),
        8,
        scratch=[
            pltpu.VMEM((6, CX, CY, CZ), F32),
            pltpu.VMEM((CX, CY, CZ), F32),
            pltpu.SemaphoreType.DMA((5,)),
        ],
        space=pltpu.HBM,
    )
    zlo, zhi = shift_both(zlo, zhi, "gz")
    yshape = (YTOTAL, 8, CZ)
    ylo, yhi = call(pack_y, [yshape, yshape], (fields, inv, zlo, zhi), 8)
    ylo, yhi = shift_both(ylo, yhi, "gy")
    xshape = (XTOTAL, 8, CZ)
    xlo, xhi = call(pack_x, [xshape, xshape], (fields, inv, zlo, zhi, ylo, yhi), 8)
    send, pick, rank = call(requests, [(64, 256), (3, 64, 128), (8, 128)], (data,), 8)
    send, xlo, xhi = lax.optimization_barrier((send, xlo, xhi))
    xlo, xhi = shift_both(xlo, xhi, "gx")
    req = lax.all_to_all(send, ("gy", "gz"), 0, 0, tiled=True)
    big = pltpu.VMEM((2, 6, XW, 4, 8, CZ), F32)
    new_fields, answers = call(
        compute,
        [(6, CX, CY, CZ), (64, 128)],
        (fields, inv, zlo, zhi, ylo, yhi, xlo, xhi, req),
        42,
        scratch=[
            pltpu.VMEM((2, NF, XW, 4, 8, CZ), F32),
            big,
            big,
            big,
            pltpu.VMEM((2, 6, CX + 4, 2, 8, CZ), F32),
            pltpu.VMEM((2, 256, 128), F32),
            pltpu.VMEM((3, 256, 256), F32),
            pltpu.VMEM((CX + 4, 2, 8, 256), F32),
            pltpu.VMEM((2, CX // 4 + 1, 8, 256), F32),
            pltpu.VMEM((2, 2, 6, CX // 4 + 1, 8, CZ), F32),
            pltpu.VMEM((48, 128), F32),
            pltpu.VMEM((256, 256), jnp.bfloat16),
        ],
        flops=100000000,
    )
    answers = lax.all_to_all(answers, ("gy", "gz"), 0, 0, tiled=True)
    receptor_values = call(collect, (6, 128), (answers, pick, rank), 8)
    return new_fields, receptor_values


def solution(mesh):
    placed = (
        P(None, "gx", "gy", "gz"),
        P("gx", "gy", "gz"),
        P(("gx", "gy", "gz"), None),
        P(("gx", "gy", "gz"), None),
        P(("gx", "gy", "gz"), None),
    )
    return jax.shard_map(
        local,
        mesh=mesh,
        in_specs=placed,
        out_specs=(P(None, "gx", "gy", "gz"), P(None, ("gx", "gy", "gz"))),
        check_vma=False,
    )
```

```python
import jax
import jax.numpy as jnp
from jax import lax
from jax.experimental import pallas as pl
from jax.experimental.pallas import tpu as pltpu
from jax.sharding import PartitionSpec as P

STEP = 0.25
CX, CY, CZ = 16, 16, 128
GX, GZ = 10, 10
NF = 7
PAIRS = NF * CX
ZGROUPS = CX // 2 + 2
XW = CX + 2 * GX
STRIDE = 20
EXACT = lax.Precision.HIGHEST
F32 = jnp.float32


def band_of(t, d=0):
    return pl.ds(8 + 8 * t + d, 8)


def z_slot(c, x):
    return (x // 2, (x % 2) * 6 + c) if c < 6 else (CX // 2 + x // 8, x % 8)


def x_lists():
    main = []
    for k in range(1, 5):
        main += [(k, c, t) for c in range(NF) for t in (0, 1, 2, 3)]
    for k in range(5, 7):
        main += [(k, c, t) for c in range(NF) for t in (1, 2, 4)]
    for k in range(7, 9):
        main += [(k, c, t) for c in range(NF) for t in (1, 2)]
        main += [(k, c, 4) for c in (0, 3)]
    for k in range(9, 11):
        main += [(k, c, t) for c in (1, 2, 4, 5) for t in (1, 2)]
    ends = []
    for q in range(5):
        ends += [(q, t, e) for t in ((0, 1, 2, 3), (0, 1, 2, 3), (1, 2, 4), (1, 2, 4), (1, 2))[q] for e in (0, 1)]
    ends += [(5, t, e) for t in (0, 1, 2, 3) for e in (0, 1)]
    return main, ends


XMAIN, XENDS = x_lists()
XROWS = len(XMAIN)
XEND = {key: XROWS + n for n, key in enumerate(XENDS)}
XTOTAL = XROWS + len(XENDS)
YTOTAL = PAIRS + 2 * ZGROUPS


def roll(value, shift, axis):
    size = value.shape[axis]
    shift = shift % size
    return value if shift == 0 else pltpu.roll(value, shift, axis)


def lanes(shape):
    return lax.broadcasted_iota(jnp.int32, shape, len(shape) - 1)


def rows_of(shape):
    return lax.broadcasted_iota(jnp.int32, shape, len(shape) - 2)


def vmem(count):
    return [pl.BlockSpec(memory_space=pltpu.VMEM)] * count


def call(body, outs, ins, limit, scratch=(), flops=1000000, space=pltpu.VMEM, first=pltpu.VMEM):
    many = isinstance(outs, list)
    return pl.pallas_call(
        body,
        out_shape=[jax.ShapeDtypeStruct(s, F32) for s in outs] if many else jax.ShapeDtypeStruct(outs, F32),
        in_specs=[pl.BlockSpec(memory_space=space)] * len(ins),
        out_specs=[pl.BlockSpec(memory_space=first)] + vmem(len(outs) - 1) if many else vmem(1)[0],
        scratch_shapes=list(scratch),
        compiler_params=pltpu.CompilerParams(vmem_limit_bytes=limit * 1048576),
        cost_estimate=pl.CostEstimate(flops=flops, bytes_accessed=1000000, transcendentals=0),
    )(*ins)


def pack_z(f_hbm, e_hbm, lo_ref, hi_ref, inv_ref, f_ref, e_ref, sems):
    copies = [pltpu.make_async_copy(e_hbm, e_ref, sems.at[0])]
    for g in range(4):
        part = pl.ds(4 * g, 4)
        copies.append(pltpu.make_async_copy(f_hbm.at[:, part], f_ref.at[:, part], sems.at[g + 1]))
    for copy in copies:
        copy.start()
    lane = lanes((CY, CZ))
    sums = {}

    def add(c, x, tile):
        g, s = z_slot(c, x)
        for side, keep in ((0, lane < GZ), (1, lane >= CZ - GZ)):
            part = roll(jnp.where(keep, tile, 0.0), GZ * (s + 1), 1)
            sums[g, side] = sums[g, side] + part if (g, side) in sums else part

    copies[0].wait()
    inv_ref[...] = 1.0 / e_ref[...]
    for x in range(CX):
        add(6, x, inv_ref[x])
    for g in range(4):
        copies[g + 1].wait()
        for x in range(4 * g, 4 * g + 4):
            for c in range(6):
                add(c, x, f_ref[c, x])
    for g in range(ZGROUPS):
        lo_ref[g] = sums[g, 0]
        hi_ref[g] = sums[g, 1]


def pack_y(f_ref, inv_ref, zlo_ref, zhi_ref, lo_ref, hi_ref):
    for out, start in ((lo_ref, 0), (hi_ref, 8)):
        rows = pl.ds(start, 8)
        for p in range(PAIRS):
            c, x = divmod(p, CX)
            out[p] = f_ref[c, x, rows] if c < 6 else inv_ref[x, rows]
        for g in range(ZGROUPS):
            out[PAIRS + g] = zlo_ref[g, rows]
            out[PAIRS + ZGROUPS + g] = zhi_ref[g, rows]


def z_ends(lo, hi, s, lane):
    first = lane < GZ * (s + 1) if s < 11 else (lane >= GZ * s) & (lane < GZ * (s + 1))
    moved = roll(jnp.where(first, lo, hi), CZ - GZ - GZ * s, 1)
    return jnp.where((lane < GZ) | (lane >= CZ - GZ), moved, 0.0)


def pack_x(f_ref, inv_ref, zlo_ref, zhi_ref, ylo_ref, yhi_ref, lo_ref, hi_ref):
    row = rows_of((8, CZ))

    def main_of(c, x, t):
        if t == 4:
            return jnp.where(row >= 4, main_of(c, x, 0), main_of(c, x, 3))
        if t in (1, 2):
            rows = pl.ds(8 * (t - 1), 8)
            return f_ref[c, x, rows] if c < 6 else inv_ref[x, rows]
        return (ylo_ref if t == 0 else yhi_ref)[c * CX + x]

    def end_of(g, t, e):
        if t == 4:
            return jnp.where(row >= 4, end_of(g, 0, e), end_of(g, 3, e))
        if t in (1, 2):
            return (zhi_ref if e else zlo_ref)[g, pl.ds(8 * (t - 1), 8)]
        return (ylo_ref if t == 0 else yhi_ref)[PAIRS + e * ZGROUPS + g]

    for out, side in ((lo_ref, 0), (hi_ref, 1)):
        for n, (k, c, t) in enumerate(XMAIN):
            out[n] = main_of(c, CX - k if side else k - 1, t)
        for (q, t, e), n in XEND.items():
            g = CX // 2 + side if q == 5 else (CX // 2 - 1 - q if side else q)
            out[n] = end_of(g, t, e)


def taylor(source, inv_ref, band, x, tiles, scale, put, comps=(0, 1, 2, 3, 4, 5), skip=0):
    row = rows_of((8, CZ))
    def load(half, c, t, d=0, e=0):
        return source[half, c, x + d - skip, band_of(t, e)]

    def dx(c):
        return {
            (half, t): (
                load(half, c, t, 1) - load(half, c, t, -1),
                load(half, c, t, 2) - load(half, c, t, -2),
            )
            for half in (0, 1)
            for t in tiles
        }

    def dy(c):
        return {
            (half, t): (
                load(half, c, t, 0, 1) - load(half, c, t, 0, -1),
                load(half, c, t, 0, 2) - load(half, c, t, 0, -2),
            )
            for half in (0, 1)
            for t in tiles
        }

    def all_dz(fields):
        block = jnp.concatenate(
            [jnp.concatenate([load(0, c, t), load(1, c, t)], axis=1) for c in fields for t in tiles], axis=0
        )
        high, middle, low = three_parts(block)
        total = jnp.dot(
            jnp.concatenate([low, middle, high], axis=1), band[...], preferred_element_type=F32
        )
        out = {}
        for i, c in enumerate(fields):
            for j, t in enumerate(tiles):
                start = 8 * (i * len(tiles) + j)
                for half in (0, 1):
                    out[c, half, t] = total[start:start + 8, 128 * half:128 * half + 128]
        return out

    pairs = ((dy, 5, 4, 0), (None, 3, 5, dx), (dx, 4, 3, dy), (None, 1, 2, dy), (dx, 2, 0, 0), (dy, 0, 1, dx))
    along_z = all_dz([c for c in (4, 3, 1, 0) if {4: 0, 3: 1, 1: 3, 0: 4}[c] in comps])
    factors = {}
    for half in (0, 1):
        for t in tiles:
            inv = inv_ref[half, 6, x, band_of(t)]
            factors[half, t] = (inv * scale, jnp.where(inv > 0.0, scale, 0.0))
    for c in comps:
        first, c1, c2, second = pairs[c]
        plus = first(c1) if first else None
        minus = second(c2) if second else None
        for key in factors:
            if plus and minus:
                rate = 8.0 * (plus[key][0] - minus[key][0]) - (plus[key][1] - minus[key][1])
            elif plus:
                rate = 8.0 * plus[key][0] - plus[key][1] - along_z[(c2,) + key]
            else:
                rate = along_z[(c1,) + key] - (8.0 * minus[key][0] - minus[key][1])
            put(key[0], c, key[1], factors[key][c // 3] * rate)


def dot(a, b, da=1, db=0):
    return lax.dot_general(a, b, (((da,), (db,)), ((), ())), precision=EXACT, preferred_element_type=F32)


def three_parts(value):
    high = value.astype(jnp.bfloat16)
    rest = value - high.astype(F32)
    middle = rest.astype(jnp.bfloat16)
    return high, middle, (rest - middle.astype(F32)).astype(jnp.bfloat16)


def split_dot(a, b):
    ah, am, al = three_parts(a)
    bh, bm, bl = three_parts(b)
    return jnp.dot(
        jnp.concatenate([al, ah, am, am, ah, ah], axis=1),
        jnp.concatenate([bh, bl, bm, bh, bm, bh], axis=0),
        preferred_element_type=F32,
    )


def spread(count, parity):
    shape = (count, 128)
    return (lanes(shape) == rows_of(shape) + parity * 64).astype(F32)


def compute(
    f_ref, own_inv_ref, zlo_ref, zhi_ref, ylo_ref, yhi_ref, xlo_ref, xhi_ref, req_ref,
    new_ref, ans_ref,
    full, t1, t2, t3, acc, words, wz, wxy, spill, edge_rows, parts, band, sems,
):
    lane = lanes((8, CZ))
    row = rows_of((8, CZ))
    zero = jnp.zeros((8, CZ), F32)
    for p in range(PAIRS):
        c, x = divmod(p, CX)
        g, s = z_slot(c, x)
        for t in (1, 2):
            own = pl.ds(8 * (t - 1), 8)
            full[0, c, GX + x, band_of(t)] = f_ref[c, x, own] if c < 6 else own_inv_ref[x, own]
            full[1, c, GX + x, band_of(t)] = z_ends(zlo_ref[g, own], zhi_ref[g, own], s, lane)
        for ref, t in ((ylo_ref, 0), (yhi_ref, 3)):
            full[0, c, GX + x, band_of(t)] = ref[p]
            full[1, c, GX + x, band_of(t)] = z_ends(ref[PAIRS + g], ref[PAIRS + ZGROUPS + g], s, lane)
    for side in (0, 1):
        ref = xhi_ref if side == 0 else xlo_ref
        where_main = {key: n for n, key in enumerate(XMAIN)}
        for k in range(1, GX + 1):
            x = GX + CX + k - 1 if side == 0 else GX - k
            for c in range(NF):
                if k > 8 and c in (0, 3, 6):
                    continue
                g, s = z_slot(c, k - 1 if side == 0 else CX - k)
                q = 5 if c == 6 else (k - 1) // 2
                done = set()
                for t in (0, 1, 2, 3, 4):
                    pair = [None, None]
                    if (k, c, t) in where_main:
                        pair[0] = ref[where_main[k, c, t]]
                    if (q, t, 0) in XEND:
                        pair[1] = z_ends(ref[XEND[q, t, 0]], ref[XEND[q, t, 1]], s, lane)
                    for half in (0, 1):
                        if pair[half] is None:
                            continue
                        if t == 4:
                            full[half, c, x, band_of(0)] = jnp.where(row >= 4, pair[half], 0.0)
                            full[half, c, x, band_of(3)] = jnp.where(row >= 4, 0.0, pair[half])
                            done |= {(half, 0), (half, 3)}
                        else:
                            full[half, c, x, band_of(t)] = pair[half]
                            done.add((half, t))
                for half in (0, 1):
                    for t in (0, 3):
                        if (half, t) not in done:
                            full[half, c, x, band_of(t)] = zero

    ring = (rows_of((256, 256)) - lanes((256, 256)) + 256) % 256
    one = lambda d: (ring == d % 256).astype(F32)
    stencil = (8.0 * (one(1) - one(-1)) + one(-2) - one(2)).astype(jnp.bfloat16)
    for i in range(3):
        band[pl.ds(256 * i, 256), :] = stencil

    for power, source, target in ((1, full, t1), (2, t1, t2), (3, t2, t3)):
        scale = STEP / power / 12.0

        def body(x, carry, source=source, target=target, scale=scale, power=power):
            def put(half, c, t, value):
                target[half, c, x - 2 * power, band_of(t)] = value

            taylor(source, full, band, x, (0, 1, 2, 3), scale, put, skip=2 * power - 2)
            return carry

        def edge(i, carry, source=source, target=target, scale=scale, power=power):
            x = jnp.where(i < 2, 2 * power + i, XW - 2 * power - 4 + i)

            def put(half, c, t, value):
                target[half, c, x - 2 * power, band_of(t)] = value

            taylor(source, full, band, x, (1, 2), scale, put, (1, 2, 4, 5), skip=2 * power - 2)
            return carry

        lax.fori_loop(0, 4, edge, 0, unroll=2)
        lax.fori_loop(2 * power + 2, XW - 2 * power - 2, body, 0, unroll=4)

    def last(x, carry):
        def put(half, c, t, value):
            total = full[half, c, x, band_of(t)] + t1[half, c, x - 2, band_of(t)]
            total = total + t2[half, c, x - 4, band_of(t)]
            total = total + t3[half, c, x - 6, band_of(t)]
            acc[half, c, x - 8, t - 1] = total + value

        taylor(t3, full, band, x, (1, 2), STEP / 4 / 12.0, put, skip=6)
        return carry

    lax.fori_loop(8, XW - 8, last, 0, unroll=4)
    writes = [
        pltpu.make_async_copy(acc.at[0, :, pl.ds(2, CX), t], new_ref.at[:, :, pl.ds(8 * t, 8), :], sems.at[t])
        for t in (0, 1)
    ]
    for write in writes:
        write.start()

    req = req_ref[...]
    words[0] = dot(req, spread(64, 0), 0, 0)
    words[1] = dot(req, spread(64, 1), 0, 0)

    def word(pair, w):
        even = words[0, pl.ds(2 * pair * STRIDE + w, 1), :]
        return even + words[1, pl.ds((2 * pair + 1) * STRIDE + w, 1), :]

    cell = rows_of((CZ, 128)).astype(F32)
    low = rows_of((8, 128)).astype(F32)
    for pair in range(6):
        kind, at = divmod(pair, 2)
        columns = pl.ds(128 * at, 128)
        bx, by, bz = word(pair, 0), word(pair, 1), word(pair, 2)
        wx = [word(pair, 3 + i) for i in range(5)]
        wy = [word(pair, 8 + i) for i in range(5)]
        wz_rows = [word(pair, 13 + i) for i in range(5)]

        def weights(position, base, values):
            away = position - base
            total = jnp.zeros(away.shape, F32)
            for i in range(5):
                total = jnp.where(away == float(i), values[i], total)
            return total

        wz[kind, pl.ds(0, CZ), columns] = weights(cell + 2.0, bz, wz_rows)
        wz[kind, pl.ds(CZ, CZ), columns] = jnp.zeros((CZ, 128), F32)
        wz[kind, pl.ds(CZ, 8), columns] = weights(low + (CZ + 2.0), bz, wz_rows)
        wz[kind, pl.ds(2 * CZ - 8, 8), columns] = weights(low - 6.0, bz, wz_rows)
        in_x = [weights(jnp.full((1, 128), float(x), F32), bx, wx) for x in range(CX + 4)] if kind == 0 else []
        if kind == 0:
            for t in (0, 1):
                in_y = weights(low + (8.0 * t + 2.0), by, wy)
                for x in range(CX + 4):
                    wxy[x, t, :, columns] = in_x[x] * in_y
        else:
            pair_row = rows_of((8, 128))
            in_y = weights((pair_row % 2).astype(F32) + (16.0 if kind == 1 else 2.0), by, wy)
            for g in range(CX // 4 + 1):
                along = weights((pair_row // 2 + 4 * g).astype(F32), bx, wx)
                spill[kind - 1, g, :, columns] = along * in_y

    for kind in (0, 1):
        for half in (0, 1):
            for c in range(6):
                for g in range(CX // 4 + 1):
                    total = None
                    for i in range(4):
                        tile = acc[half, c, 4 * g + i, 1 - kind]
                        moved = roll(tile, 2 * i - (6 if kind == 0 else 0), 0)
                        total = moved if total is None else jnp.where(row >= 2 * i, moved, total)
                    edge_rows[kind, half, c, g] = total

    parts[...] = jnp.zeros((48, 128), F32)
    for kind in range(3):
        grid = [acc[half] if kind == 0 else edge_rows[kind - 1, half] for half in (0, 1)]
        weight = wxy[...].reshape(-1, 256) if kind == 0 else spill[kind - 1].reshape(-1, 256)
        along = split_dot(jnp.concatenate([g.reshape(-1, CZ) for g in grid], axis=1), wz[kind])
        count = weight.shape[0]
        for c in range(6):
            total = jnp.sum(along[c * count:c * count + count] * weight, axis=0, keepdims=True)
            for at in (0, 1):
                parts[pl.ds((2 * kind + at) * 8 + c, 1), :] = total[:, 128 * at:128 * at + 128]
    values = parts[...]
    blank = jnp.zeros((16, 128), F32)
    filled = jnp.concatenate([values, blank], axis=0)
    empty = jnp.zeros((64, 128), F32)
    ans_ref[...] = dot(spread(64, 0), jnp.concatenate([filled, empty], axis=0), 1, 1) + dot(
        spread(64, 1), jnp.concatenate([empty, filled], axis=0), 1, 1
    )
    for write in writes:
        write.wait()


def requests(data_ref, send_ref, pick_ref, rank_ref):
    data = data_ref[...]
    wide = (128, 128)
    owner = jnp.broadcast_to(data[:, 18:19], wide)
    base_y = jnp.broadcast_to(data[:, 1:2], wide)
    r, q = rows_of(wide), lanes(wide)
    owner_row = jnp.sum(jnp.where(r == q, owner, 0.0), axis=0, keepdims=True)
    base_row = jnp.sum(jnp.where(r == q, base_y, 0.0), axis=0, keepdims=True)
    same = owner == owner_row
    rank_col = jnp.sum(jnp.where(same & (q < r), 1.0, 0.0), axis=1, keepdims=True)
    rank_row = jnp.sum(jnp.where(same & (r < q), 1.0, 0.0), axis=0, keepdims=True)
    rank_ref[...] = jnp.broadcast_to(rank_row, (8, 128))

    lane = lanes((128, 256))
    slot, w = lane // STRIDE, lane % STRIDE
    word_row = rows_of((128, 256))
    copies = jnp.where((lanes((128, 256)) % STRIDE == word_row) & (word_row < 18) & (lane < 12 * STRIDE), 1.0, 0.0)
    spread_out = dot(data, copies)
    moved = jnp.where(w == 1, jnp.where(slot // 4 == 1, float(CY), jnp.where(slot // 4 == 2, -float(CY), 0.0)), 0.0)
    chosen = (slot % 4).astype(F32) == rank_col
    spread_out = jnp.where(chosen, spread_out + moved, 0.0)

    place = rows_of((64, 128)).astype(F32)
    total = jnp.zeros((64, 256), F32)
    for kind, move in ((0, 0.0), (1, -16.0), (2, 16.0)):
        hit = place == owner_row + move
        if kind == 1:
            hit = hit & (base_row < 2.0)
        if kind == 2:
            hit = hit & (base_row > 13.0)
        pick = jnp.where(hit, 1.0, 0.0)
        pick_ref[kind] = pick
        total = total + dot(pick, jnp.where(slot // 4 == kind, spread_out, 0.0))
    send_ref[...] = total


def collect(ans_ref, pick_ref, rank_ref, out_ref):
    ans = ans_ref[...]
    rank = rank_ref[...]
    total = jnp.zeros((8, 128), F32)
    for kind in range(3):
        got = dot(ans, pick_ref[kind], 0, 0)
        for j in range(4):
            start = (j % 2) * 64 + (2 * kind + j // 2) * 8
            total = total + jnp.where(rank == float(j), got[start:start + 8], 0.0)
    out_ref[...] = total[0:6]


def shift_both(low_edge, high_edge, axis):
    size = lax.axis_size(axis)
    up = [(i, i + 1) for i in range(size - 1)]
    down = [(i + 1, i) for i in range(size - 1)]
    return lax.ppermute(high_edge, axis, up), lax.ppermute(low_edge, axis, down)


def local(fields, permittivity, donor_owner, donor_base, donor_weights):
    data = jnp.concatenate(
        [
            donor_base.astype(F32),
            donor_weights,
            donor_owner.astype(F32),
            jnp.zeros((donor_owner.shape[0], 128 - 19), F32),
        ],
        axis=1,
    )
    zshape = (ZGROUPS, CY, CZ)
    zlo, zhi, inv = call(
        pack_z,
        [zshape, zshape, (CX, CY, CZ)],
        (fields, permittivity),
        53,
        scratch=[
            pltpu.VMEM((6, CX, CY, CZ), F32),
            pltpu.VMEM((CX, CY, CZ), F32),
            pltpu.SemaphoreType.DMA((5,)),
        ],
        space=pltpu.HBM,
    )
    zlo, zhi = shift_both(zlo, zhi, "gz")
    yshape = (YTOTAL, 8, CZ)
    ylo, yhi = call(pack_y, [yshape, yshape], (fields, inv, zlo, zhi), 8)
    ylo, yhi = shift_both(ylo, yhi, "gy")
    xshape = (XTOTAL, 8, CZ)
    xlo, xhi = call(pack_x, [xshape, xshape], (fields, inv, zlo, zhi, ylo, yhi), 8)
    send, pick, rank = call(requests, [(64, 256), (3, 64, 128), (8, 128)], (data,), 8)
    send, xlo, xhi = lax.optimization_barrier((send, xlo, xhi))
    xlo, xhi = shift_both(xlo, xhi, "gx")
    req = lax.all_to_all(send, ("gy", "gz"), 0, 0, tiled=True)
    new_fields, answers = call(
        compute,
        [(6, CX, CY, CZ), (64, 128)],
        (fields, inv, zlo, zhi, ylo, yhi, xlo, xhi, req),
        46,
        scratch=[
            pltpu.VMEM((2, NF, XW, 48, CZ), F32),
            *[pltpu.VMEM((2, 6, XW - 4 * m, 48, CZ), F32) for m in (1, 2, 3)],
            pltpu.VMEM((2, 6, CX + 4, 2, 8, CZ), F32),
            pltpu.VMEM((2, 256, 128), F32),
            pltpu.VMEM((3, 256, 256), F32),
            pltpu.VMEM((CX + 4, 2, 8, 256), F32),
            pltpu.VMEM((2, CX // 4 + 1, 8, 256), F32),
            pltpu.VMEM((2, 2, 6, CX // 4 + 1, 8, CZ), F32),
            pltpu.VMEM((48, 128), F32),
            pltpu.VMEM((768, 256), jnp.bfloat16),
            pltpu.SemaphoreType.DMA((2,)),
        ],
        flops=100000000,
        first=pl.ANY,
    )
    answers = lax.all_to_all(answers, ("gy", "gz"), 0, 0, tiled=True)
    receptor_values = call(collect, (6, 128), (answers, pick, rank), 8)
    return new_fields, receptor_values


def solution(mesh):
    placed = (
        P(None, "gx", "gy", "gz"),
        P("gx", "gy", "gz"),
        P(("gx", "gy", "gz"), None),
        P(("gx", "gy", "gz"), None),
        P(("gx", "gy", "gz"), None),
    )
    return jax.shard_map(
        local,
        mesh=mesh,
        in_specs=placed,
        out_specs=(P(None, "gx", "gy", "gz"), P(None, ("gx", "gy", "gz"))),
        check_vma=False,
    )
```

```python
import jax
import jax.numpy as jnp
from jax import lax
from jax.experimental import pallas as pl
from jax.experimental.pallas import tpu as pltpu
from jax.sharding import PartitionSpec as P

STEP = 0.25
CX, CY, CZ = 16, 16, 128
GX, GZ = 10, 10
NF = 7
PAIRS = NF * CX
ZGROUPS = CX // 2 + 2
XW = CX + 2 * GX
STRIDE = 20
ROWS = 4
EXACT = lax.Precision.HIGHEST
F32 = jnp.float32


def band_of(t, d=0):
    return pl.ds(8 + 8 * t + d, 8)


def z_slot(c, x):
    return (x // 2, (x % 2) * 6 + c) if c < 6 else (CX // 2 + x // 8, x % 8)


def x_lists():
    main = []
    for k in range(1, 5):
        main += [(k, c, t) for c in range(NF) for t in (0, 1, 2, 3)]
    for k in range(5, 7):
        main += [(k, c, t) for c in range(NF) for t in (1, 2, 4)]
    for k in range(7, 9):
        main += [(k, c, t) for c in range(NF) for t in (1, 2)]
        main += [(k, c, 4) for c in (0, 3)]
    for k in range(9, 11):
        main += [(k, c, t) for c in (1, 2, 4, 5) for t in (1, 2)]
    ends = []
    for q in range(5):
        ends += [(q, t, e) for t in ((0, 1, 2, 3), (0, 1, 2, 3), (1, 2, 4), (1, 2, 4), (1, 2))[q] for e in (0, 1)]
    ends += [(5, t, e) for t in (0, 1, 2, 3) for e in (0, 1)]
    return main, ends


XMAIN, XENDS = x_lists()
XROWS = len(XMAIN)
XEND = {key: XROWS + n for n, key in enumerate(XENDS)}
XTOTAL = XROWS + len(XENDS)
YTOTAL = PAIRS + 2 * ZGROUPS


def roll(value, shift, axis):
    size = value.shape[axis]
    shift = shift % size
    return value if shift == 0 else pltpu.roll(value, shift, axis)


def lanes(shape):
    return lax.broadcasted_iota(jnp.int32, shape, len(shape) - 1)


def rows_of(shape):
    return lax.broadcasted_iota(jnp.int32, shape, len(shape) - 2)


def vmem(count):
    return [pl.BlockSpec(memory_space=pltpu.VMEM)] * count


def call(body, outs, ins, limit, scratch=(), flops=1000000, space=pltpu.VMEM, first=pltpu.VMEM):
    many = isinstance(outs, list)
    return pl.pallas_call(
        body,
        out_shape=[jax.ShapeDtypeStruct(s, jnp.bfloat16 if s == (4, 256, 256) else F32) for s in outs]
        if many
        else jax.ShapeDtypeStruct(outs, F32),
        in_specs=[pl.BlockSpec(memory_space=space)] * len(ins),
        out_specs=[pl.BlockSpec(memory_space=first)] + vmem(len(outs) - 1) if many else vmem(1)[0],
        scratch_shapes=list(scratch),
        compiler_params=pltpu.CompilerParams(vmem_limit_bytes=limit * 1048576),
        cost_estimate=pl.CostEstimate(flops=flops, bytes_accessed=1000000, transcendentals=0),
    )(*ins)


def pack_z(f_hbm, e_hbm, lo_ref, hi_ref, inv_ref, f_ref, e_ref, sems):
    copies = [pltpu.make_async_copy(e_hbm, e_ref, sems.at[0])]
    for g in range(4):
        part = pl.ds(4 * g, 4)
        copies.append(pltpu.make_async_copy(f_hbm.at[:, part], f_ref.at[:, part], sems.at[g + 1]))
    for copy in copies:
        copy.start()
    lane = lanes((CY, CZ))
    sums = {}

    def add(c, x, tile):
        g, s = z_slot(c, x)
        for side, keep in ((0, lane < GZ), (1, lane >= CZ - GZ)):
            part = roll(jnp.where(keep, tile, 0.0), GZ * (s + 1), 1)
            sums[g, side] = sums[g, side] + part if (g, side) in sums else part

    copies[0].wait()
    inv_ref[...] = 1.0 / e_ref[...]
    for x in range(CX):
        add(6, x, inv_ref[x])
    for g in range(4):
        copies[g + 1].wait()
        for x in range(4 * g, 4 * g + 4):
            for c in range(6):
                add(c, x, f_ref[c, x])
    for g in range(ZGROUPS):
        lo_ref[g] = sums[g, 0]
        hi_ref[g] = sums[g, 1]


def pack_y(f_ref, inv_ref, zlo_ref, zhi_ref, lo_ref, hi_ref):
    for out, start in ((lo_ref, 0), (hi_ref, 8)):
        rows = pl.ds(start, 8)
        for p in range(PAIRS):
            c, x = divmod(p, CX)
            out[p] = f_ref[c, x, rows] if c < 6 else inv_ref[x, rows]
        for g in range(ZGROUPS):
            out[PAIRS + g] = zlo_ref[g, rows]
            out[PAIRS + ZGROUPS + g] = zhi_ref[g, rows]


def z_ends(lo, hi, s, lane, t, total):
    first = lane < GZ * (s + 1) if s < 11 else (lane >= GZ * s) & (lane < GZ * (s + 1))
    moved = roll(jnp.where(first, lo, hi), 32 * t - GZ * s, 1)
    return jnp.where((lane >= 32 * t) & (lane < 32 * t + 2 * GZ), moved, total)


def pack_x(f_ref, inv_ref, zlo_ref, zhi_ref, ylo_ref, yhi_ref, lo_ref, hi_ref):
    row = rows_of((8, CZ))

    def main_of(c, x, t):
        if t == 4:
            return jnp.where(row >= 4, main_of(c, x, 0), main_of(c, x, 3))
        if t in (1, 2):
            rows = pl.ds(8 * (t - 1), 8)
            return f_ref[c, x, rows] if c < 6 else inv_ref[x, rows]
        return (ylo_ref if t == 0 else yhi_ref)[c * CX + x]

    def end_of(g, t, e):
        if t == 4:
            return jnp.where(row >= 4, end_of(g, 0, e), end_of(g, 3, e))
        if t in (1, 2):
            return (zhi_ref if e else zlo_ref)[g, pl.ds(8 * (t - 1), 8)]
        return (ylo_ref if t == 0 else yhi_ref)[PAIRS + e * ZGROUPS + g]

    for out, side in ((lo_ref, 0), (hi_ref, 1)):
        for n, (k, c, t) in enumerate(XMAIN):
            out[n] = main_of(c, CX - k if side else k - 1, t)
        for (q, t, e), n in XEND.items():
            g = CX // 2 + side if q == 5 else (CX // 2 - 1 - q if side else q)
            out[n] = end_of(g, t, e)


def taylor(source, packed, inv_main, inv_packed, band, xs, tiles, scale, put, comps=(0, 1, 2, 3, 4, 5), skip=0):
    fields = [c for c in (4, 3, 1, 0) if {4: 0, 3: 1, 1: 3, 0: 4}[c] in comps]
    keys = [(i, c) for i in range(len(xs)) for c in fields]
    ghosts = three_parts(jnp.concatenate([packed[c, xs[i] - skip, pl.ds(8, 8)] for i, c in keys], axis=0))
    along_z = {}
    for t in tiles:
        mains = three_parts(jnp.concatenate([source[c, xs[i] - skip, band_of(t)] for i, c in keys], axis=0))
        left = [part for n in (2, 1, 0) for part in (mains[n], ghosts[n])]
        total = jnp.dot(jnp.concatenate(left, axis=1), jnp.concatenate([band[t]] * 3, axis=0), preferred_element_type=F32)
        for n, key in enumerate(keys):
            along_z[key + (t,)] = total[8 * n:8 * n + 8, 0:128]
            part = total[8 * n:8 * n + 8, 128:256]
            along_z[key + (4,)] = along_z[key + (4,)] + part if key + (4,) in along_z else part
    for i, x in enumerate(xs):
        for t in tuple(tiles) + (4,):
            one_tile(packed if t == 4 else source, inv_packed if t == 4 else inv_main, along_z, i, x, t, scale, put, comps, skip)


def one_tile(source, inv_ref, along_z, i, x, t, scale, put, comps, skip):
    def load(c, d=0, e=0):
        return source[c, x + d - skip, pl.ds(8 + e, 8) if t == 4 else band_of(t, e)]

    def dx(c):
        return load(c, 1) - load(c, -1), load(c, 2) - load(c, -2)

    def dy(c):
        return load(c, 0, 1) - load(c, 0, -1), load(c, 0, 2) - load(c, 0, -2)

    pairs = ((dy, 5, 4, 0), (None, 3, 5, dx), (dx, 4, 3, dy), (None, 1, 2, dy), (dx, 2, 0, 0), (dy, 0, 1, dx))
    inv = inv_ref[6, x, pl.ds(8, 8) if t == 4 else band_of(t)]
    factors = (inv * scale, jnp.where(inv > 0.0, scale, 0.0))
    for c in comps:
        first, c1, c2, second = pairs[c]
        if first and second:
            plus, minus = first(c1), second(c2)
            rate = 8.0 * (plus[0] - minus[0]) - (plus[1] - minus[1])
        elif first:
            plus = first(c1)
            rate = 8.0 * plus[0] - plus[1] - along_z[i, c2, t]
        else:
            minus = second(c2)
            rate = along_z[i, c1, t] - (8.0 * minus[0] - minus[1])
        put(c, x, t, factors[c // 3] * rate)


def store_packed(ref, c, x, value):
    ref[c, x, pl.ds(8, 8)] = value
    if c in (0, 2, 3, 5):
        ref[c, x, pl.ds(0, 8)] = roll(value, 32, 1)
        ref[c, x, pl.ds(16, 8)] = roll(value, -32, 1)


def packed_z(lane, t):
    place = lane - 32 * t
    inside = (place >= 0) & (place < 2 * GZ)
    return jnp.where(inside, jnp.where(place < GZ, place - GZ, place + (CZ - GZ)), -1000)


def dot(a, b, da=1, db=0):
    return lax.dot_general(a, b, (((da,), (db,)), ((), ())), precision=EXACT, preferred_element_type=F32)


def three_parts(value):
    high = value.astype(jnp.bfloat16)
    rest = value - high.astype(F32)
    middle = rest.astype(jnp.bfloat16)
    return high, middle, (rest - middle.astype(F32)).astype(jnp.bfloat16)


def split_dot(a, b):
    ah, am, al = three_parts(a)
    bh, bm, bl = three_parts(b)
    return jnp.dot(
        jnp.concatenate([al, ah, am, am, ah, ah], axis=1),
        jnp.concatenate([bh, bl, bm, bh, bm, bh], axis=0),
        preferred_element_type=F32,
    )


def spread(count, parity):
    shape = (count, 128)
    return (lanes(shape) == rows_of(shape) + parity * 64).astype(F32)


def compute(
    f_ref, own_inv_ref, zlo_ref, zhi_ref, ylo_ref, yhi_ref, xlo_ref, xhi_ref, req_ref, band,
    new_ref, ans_ref,
    full, full_p, t1, t2, t3, p1, p2, p3, acc, acc_p, words, wz, wxy, spill, edge_rows, parts, sems,
):
    lane = lanes((8, CZ))
    row = rows_of((8, CZ))
    zero = jnp.zeros((8, CZ), F32)
    for p in range(PAIRS):
        c, x = divmod(p, CX)
        g, s = z_slot(c, x)
        total = zero
        for t in (0, 1, 2, 3):
            if t in (1, 2):
                own = pl.ds(8 * (t - 1), 8)
                full[c, GX + x, band_of(t)] = f_ref[c, x, own] if c < 6 else own_inv_ref[x, own]
                lo, hi = zlo_ref[g, own], zhi_ref[g, own]
            else:
                ref = ylo_ref if t == 0 else yhi_ref
                full[c, GX + x, band_of(t)] = ref[p]
                lo, hi = ref[PAIRS + g], ref[PAIRS + ZGROUPS + g]
            total = z_ends(lo, hi, s, lane, t, total)
        store_packed(full_p, c, GX + x, total)
    for side in (0, 1):
        ref = xhi_ref if side == 0 else xlo_ref
        where_main = {key: n for n, key in enumerate(XMAIN)}
        for k in range(1, GX + 1):
            x = GX + CX + k - 1 if side == 0 else GX - k
            for c in range(NF):
                if k > 8 and c in (0, 3, 6):
                    continue
                g, s = z_slot(c, k - 1 if side == 0 else CX - k)
                q = 5 if c == 6 else (k - 1) // 2
                mains = [zero, zero, zero, zero]
                total = zero
                for t in (0, 1, 2, 3, 4):
                    if (k, c, t) in where_main:
                        value = ref[where_main[k, c, t]]
                        if t == 4:
                            mains[0], mains[3] = jnp.where(row >= 4, value, 0.0), jnp.where(row >= 4, 0.0, value)
                        else:
                            mains[t] = value
                    if (q, t, 0) in XEND:
                        lo, hi = ref[XEND[q, t, 0]], ref[XEND[q, t, 1]]
                        if t == 4:
                            top = z_ends(lo, hi, s, lane, 0, zero)
                            bottom = z_ends(lo, hi, s, lane, 3, zero)
                            total = total + jnp.where(row >= 4, top, bottom)
                        else:
                            total = z_ends(lo, hi, s, lane, t, total)
                for t in range(4):
                    full[c, x, band_of(t)] = mains[t]
                store_packed(full_p, c, x, total)

    for power, source, packed, target, target_p in (
        (1, full, full_p, t1, p1), (2, t1, p1, t2, p2), (3, t2, p2, t3, p3)
    ):
        scale, skip = STEP / power / 12.0, 2 * power - 2

        def put(c, x, t, value, target=target, target_p=target_p, power=power):
            if t == 4:
                store_packed(target_p, c, x - 2 * power, value)
            else:
                target[c, x - 2 * power, band_of(t)] = value

        def body(i, carry, source=source, packed=packed, scale=scale, skip=skip, put=put, power=power):
            xs = [2 * power + 2 + ROWS * i + j for j in range(ROWS)]
            taylor(source, packed, full, full_p, band, xs, (0, 1, 2, 3), scale, put, skip=skip)
            return carry

        ends = [2 * power, 2 * power + 1, XW - 2 * power - 2, XW - 2 * power - 1]
        taylor(source, packed, full, full_p, band, ends, (1, 2), scale, put, (1, 2, 4, 5), skip)
        lax.fori_loop(0, (XW - 4 * power - 4) // ROWS, body, 0)

    def finish(c, x, t, value):
        if t == 4:
            terms = [ref[c, x - d, pl.ds(8, 8)] for ref, d in ((full_p, 0), (p1, 2), (p2, 4), (p3, 6))]
        else:
            terms = [ref[c, x - d, band_of(t)] for ref, d in ((full, 0), (t1, 2), (t2, 4), (t3, 6))]
        total = terms[0] + terms[1]
        total = total + terms[2]
        total = total + terms[3] + value
        if t == 4:
            acc_p[c, x - 8] = total
        else:
            acc[c, x - 8, t - 1] = total

    def last(i, carry):
        xs = [8 + ROWS * i + j for j in range(ROWS)]
        taylor(t3, p3, full, full_p, band, xs, (1, 2), STEP / 4 / 12.0, finish, skip=6)
        return carry

    lax.fori_loop(0, (XW - 16) // ROWS, last, 0)
    writes = [
        pltpu.make_async_copy(acc.at[:, pl.ds(2, CX), t], new_ref.at[:, :, pl.ds(8 * t, 8), :], sems.at[t])
        for t in (0, 1)
    ]
    for write in writes:
        write.start()

    req = req_ref[...]
    words[0] = dot(req, spread(64, 0), 0, 0)
    words[1] = dot(req, spread(64, 1), 0, 0)

    def word(pair, w):
        even = words[0, pl.ds(2 * pair * STRIDE + w, 1), :]
        return even + words[1, pl.ds((2 * pair + 1) * STRIDE + w, 1), :]

    cell = rows_of((CZ, 128)).astype(F32)
    low = rows_of((8, 128)).astype(F32)
    for pair in range(6):
        kind, at = divmod(pair, 2)
        columns = pl.ds(128 * at, 128)
        bx, by, bz = word(pair, 0), word(pair, 1), word(pair, 2)
        wx = [word(pair, 3 + i) for i in range(5)]
        wy = [word(pair, 8 + i) for i in range(5)]
        wz_rows = [word(pair, 13 + i) for i in range(5)]

        def weights(position, base, values):
            away = position - base
            total = jnp.zeros(away.shape, F32)
            for i in range(5):
                total = jnp.where(away == float(i), values[i], total)
            return total

        for t in ((1, 2), (2,), (1,))[kind]:
            use = (0, 1)[t - 1] if kind == 0 else kind + 1
            wz[use, pl.ds(0, CZ), columns] = weights(cell + 2.0, bz, wz_rows)
            ghost_z = packed_z(rows_of((CZ, 128)), t).astype(F32)
            wz[use, pl.ds(CZ, CZ), columns] = weights(ghost_z + 2.0, bz, wz_rows)
        in_x = [weights(jnp.full((1, 128), float(x), F32), bx, wx) for x in range(CX + 4)] if kind == 0 else []
        if kind == 0:
            for t in (0, 1):
                in_y = weights(low + (8.0 * t + 2.0), by, wy)
                for x in range(CX + 4):
                    wxy[x, t, :, columns] = in_x[x] * in_y
        else:
            pair_row = rows_of((8, 128))
            in_y = weights((pair_row % 2).astype(F32) + (16.0 if kind == 1 else 2.0), by, wy)
            for g in range(CX // 4 + 1):
                along = weights((pair_row // 2 + 4 * g).astype(F32), bx, wx)
                spill[kind - 1, g, :, columns] = along * in_y

    for kind in (0, 1):
        for half in (0, 1):
            for c in range(6):
                for g in range(CX // 4 + 1):
                    total = None
                    for i in range(4):
                        value = acc_p[c, 4 * g + i] if half else acc[c, 4 * g + i, 1 - kind]
                        moved = roll(value, 2 * i - (6 if kind == 0 else 0), 0)
                        total = moved if total is None else jnp.where(row >= 2 * i, moved, total)
                    edge_rows[kind, half, c, g] = total

    parts[...] = jnp.zeros((48, 128), F32)
    sums = {}
    for use in range(4):
        kind = max(use - 1, 0)
        if kind == 0:
            grid, weight = [acc[:, :, use], acc_p[...]], wxy[:, use].reshape(-1, 256)
        else:
            grid, weight = [edge_rows[kind - 1, half] for half in (0, 1)], spill[kind - 1].reshape(-1, 256)
        along = split_dot(jnp.concatenate([g.reshape(-1, CZ) for g in grid], axis=1), wz[use])
        count = weight.shape[0]
        for c in range(6):
            total = jnp.sum(along[c * count:c * count + count] * weight, axis=0, keepdims=True)
            sums[kind, c] = sums[kind, c] + total if (kind, c) in sums else total
    for (kind, c), total in sums.items():
        for at in (0, 1):
            parts[pl.ds((2 * kind + at) * 8 + c, 1), :] = total[:, 128 * at:128 * at + 128]
    values = parts[...]
    blank = jnp.zeros((16, 128), F32)
    filled = jnp.concatenate([values, blank], axis=0)
    empty = jnp.zeros((64, 128), F32)
    ans_ref[...] = dot(spread(64, 0), jnp.concatenate([filled, empty], axis=0), 1, 1) + dot(
        spread(64, 1), jnp.concatenate([empty, filled], axis=0), 1, 1
    )
    for write in writes:
        write.wait()


def requests(data_ref, send_ref, pick_ref, rank_ref, band_ref):
    for t in range(4):
        def places(index):
            return jnp.where(index < CZ, index, packed_z(index - CZ, t))

        apart = places(rows_of((256, 256))) - places(lanes((256, 256)))
        real = (places(rows_of((256, 256))) > -900) & (places(lanes((256, 256))) > -900)
        one = lambda d: ((apart == d) & real).astype(F32)
        stencil = (8.0 * (one(1) - one(-1)) + one(-2) - one(2)).astype(jnp.bfloat16)
        band_ref[t] = stencil

    data = data_ref[...]
    wide = (128, 128)
    owner = jnp.broadcast_to(data[:, 18:19], wide)
    base_y = jnp.broadcast_to(data[:, 1:2], wide)
    r, q = rows_of(wide), lanes(wide)
    owner_row = jnp.sum(jnp.where(r == q, owner, 0.0), axis=0, keepdims=True)
    base_row = jnp.sum(jnp.where(r == q, base_y, 0.0), axis=0, keepdims=True)
    same = owner == owner_row
    rank_col = jnp.sum(jnp.where(same & (q < r), 1.0, 0.0), axis=1, keepdims=True)
    rank_row = jnp.sum(jnp.where(same & (r < q), 1.0, 0.0), axis=0, keepdims=True)
    rank_ref[...] = jnp.broadcast_to(rank_row, (8, 128))

    lane = lanes((128, 256))
    slot, w = lane // STRIDE, lane % STRIDE
    word_row = rows_of((128, 256))
    copies = jnp.where((lanes((128, 256)) % STRIDE == word_row) & (word_row < 18) & (lane < 12 * STRIDE), 1.0, 0.0)
    spread_out = dot(data, copies)
    moved = jnp.where(w == 1, jnp.where(slot // 4 == 1, float(CY), jnp.where(slot // 4 == 2, -float(CY), 0.0)), 0.0)
    chosen = (slot % 4).astype(F32) == rank_col
    spread_out = jnp.where(chosen, spread_out + moved, 0.0)

    place = rows_of((64, 128)).astype(F32)
    total = jnp.zeros((64, 256), F32)
    for kind, move in ((0, 0.0), (1, -16.0), (2, 16.0)):
        hit = place == owner_row + move
        if kind == 1:
            hit = hit & (base_row < 2.0)
        if kind == 2:
            hit = hit & (base_row > 13.0)
        pick = jnp.where(hit, 1.0, 0.0)
        pick_ref[kind] = pick
        total = total + dot(pick, jnp.where(slot // 4 == kind, spread_out, 0.0))
    send_ref[...] = total


def collect(ans_ref, pick_ref, rank_ref, out_ref):
    ans = ans_ref[...]
    rank = rank_ref[...]
    total = jnp.zeros((8, 128), F32)
    for kind in range(3):
        got = dot(ans, pick_ref[kind], 0, 0)
        for j in range(4):
            start = (j % 2) * 64 + (2 * kind + j // 2) * 8
            total = total + jnp.where(rank == float(j), got[start:start + 8], 0.0)
    out_ref[...] = total[0:6]


def shift_both(low_edge, high_edge, axis):
    size = lax.axis_size(axis)
    up = [(i, i + 1) for i in range(size - 1)]
    down = [(i + 1, i) for i in range(size - 1)]
    return lax.ppermute(high_edge, axis, up), lax.ppermute(low_edge, axis, down)


def local(fields, permittivity, donor_owner, donor_base, donor_weights):
    data = jnp.concatenate(
        [
            donor_base.astype(F32),
            donor_weights,
            donor_owner.astype(F32),
            jnp.zeros((donor_owner.shape[0], 128 - 19), F32),
        ],
        axis=1,
    )
    zshape = (ZGROUPS, CY, CZ)
    zlo, zhi, inv = call(
        pack_z,
        [zshape, zshape, (CX, CY, CZ)],
        (fields, permittivity),
        53,
        scratch=[
            pltpu.VMEM((6, CX, CY, CZ), F32),
            pltpu.VMEM((CX, CY, CZ), F32),
            pltpu.SemaphoreType.DMA((5,)),
        ],
        space=pltpu.HBM,
    )
    zlo, zhi = shift_both(zlo, zhi, "gz")
    yshape = (YTOTAL, 8, CZ)
    ylo, yhi = call(pack_y, [yshape, yshape], (fields, inv, zlo, zhi), 8)
    ylo, yhi = shift_both(ylo, yhi, "gy")
    xshape = (XTOTAL, 8, CZ)
    xlo, xhi = call(pack_x, [xshape, xshape], (fields, inv, zlo, zhi, ylo, yhi), 8)
    send, pick, rank, band = call(requests, [(64, 256), (3, 64, 128), (8, 128), (4, 256, 256)], (data,), 8)
    send, xlo, xhi = lax.optimization_barrier((send, xlo, xhi))
    xlo, xhi = shift_both(xlo, xhi, "gx")
    req = lax.all_to_all(send, ("gy", "gz"), 0, 0, tiled=True)
    new_fields, answers = call(
        compute,
        [(6, CX, CY, CZ), (64, 128)],
        (fields, inv, zlo, zhi, ylo, yhi, xlo, xhi, req, band),
        40,
        scratch=[
            pltpu.VMEM((NF, XW, 48, CZ), F32),
            pltpu.VMEM((NF, XW, 24, CZ), F32),
            *[pltpu.VMEM((6, XW - 4 * m, 48, CZ), F32) for m in (1, 2, 3)],
            *[pltpu.VMEM((6, XW - 4 * m, 24, CZ), F32) for m in (1, 2, 3)],
            pltpu.VMEM((6, CX + 4, 2, 8, CZ), F32),
            pltpu.VMEM((6, CX + 4, 8, CZ), F32),
            pltpu.VMEM((2, 256, 128), F32),
            pltpu.VMEM((4, 256, 256), F32),
            pltpu.VMEM((CX + 4, 2, 8, 256), F32),
            pltpu.VMEM((2, CX // 4 + 1, 8, 256), F32),
            pltpu.VMEM((2, 2, 6, CX // 4 + 1, 8, CZ), F32),
            pltpu.VMEM((48, 128), F32),
            pltpu.SemaphoreType.DMA((2,)),
        ],
        flops=100000000,
        first=pl.ANY,
    )
    answers = lax.all_to_all(answers, ("gy", "gz"), 0, 0, tiled=True)
    receptor_values = call(collect, (6, 128), (answers, pick, rank), 8)
    return new_fields, receptor_values


def solution(mesh):
    placed = (
        P(None, "gx", "gy", "gz"),
        P("gx", "gy", "gz"),
        P(("gx", "gy", "gz"), None),
        P(("gx", "gy", "gz"), None),
        P(("gx", "gy", "gz"), None),
    )
    return jax.shard_map(
        local,
        mesh=mesh,
        in_specs=placed,
        out_specs=(P(None, "gx", "gy", "gz"), P(None, ("gx", "gy", "gz"))),
        check_vma=False,
    )
```

```python
import jax
import jax.numpy as jnp
from jax import lax
from jax.experimental import pallas as pl
from jax.experimental.pallas import tpu as pltpu
from jax.sharding import PartitionSpec as P

STEP = 0.25
CX, CY, CZ = 16, 16, 128
GX, GZ = 10, 10
NF = 7
PAIRS = NF * CX
ZGROUPS = CX // 2 + 2
XW = CX + 2 * GX
STRIDE = 20
ROWS = 4
EXACT = lax.Precision.HIGHEST
F32 = jnp.float32


def band_of(t, d=0):
    return pl.ds(8 + 8 * t + d, 8)


def z_slot(c, x):
    return (x // 2, (x % 2) * 6 + c) if c < 6 else (CX // 2 + x // 8, x % 8)


def x_lists():
    main = []
    for k in range(1, 5):
        main += [(k, c, t) for c in range(NF) for t in (0, 1, 2, 3)]
    for k in range(5, 7):
        main += [(k, c, t) for c in range(NF) for t in (1, 2, 4)]
    for k in range(7, 9):
        main += [(k, c, t) for c in range(NF) for t in (1, 2)]
        main += [(k, c, 4) for c in (0, 3)]
    for k in range(9, 11):
        main += [(k, c, t) for c in (1, 2, 4, 5) for t in (1, 2)]
    ends = []
    for q in range(5):
        ends += [(q, t, e) for t in ((0, 1, 2, 3), (0, 1, 2, 3), (1, 2, 4), (1, 2, 4), (1, 2))[q] for e in (0, 1)]
    ends += [(5, t, e) for t in (0, 1, 2, 3) for e in (0, 1)]
    return main, ends


XMAIN, XENDS = x_lists()
XROWS = len(XMAIN)
XEND = {key: XROWS + n for n, key in enumerate(XENDS)}
XTOTAL = XROWS + len(XENDS)
YTOTAL = PAIRS + 2 * ZGROUPS


def roll(value, shift, axis):
    size = value.shape[axis]
    shift = shift % size
    return value if shift == 0 else pltpu.roll(value, shift, axis)


def lanes(shape):
    return lax.broadcasted_iota(jnp.int32, shape, len(shape) - 1)


def rows_of(shape):
    return lax.broadcasted_iota(jnp.int32, shape, len(shape) - 2)


def vmem(count):
    return [pl.BlockSpec(memory_space=pltpu.VMEM)] * count


def call(body, outs, ins, limit, scratch=(), flops=1000000, space=pltpu.VMEM, first=pltpu.VMEM):
    many = isinstance(outs, list)
    return pl.pallas_call(
        body,
        out_shape=[jax.ShapeDtypeStruct(s, jnp.bfloat16 if s == (4, 256, 256) else F32) for s in outs]
        if many
        else jax.ShapeDtypeStruct(outs, F32),
        in_specs=[pl.BlockSpec(memory_space=space)] * len(ins),
        out_specs=[pl.BlockSpec(memory_space=first)] + vmem(len(outs) - 1) if many else vmem(1)[0],
        scratch_shapes=list(scratch),
        compiler_params=pltpu.CompilerParams(vmem_limit_bytes=limit * 1048576),
        cost_estimate=pl.CostEstimate(flops=flops, bytes_accessed=1000000, transcendentals=0),
    )(*ins)


def pack_z(f_hbm, e_hbm, lo_ref, hi_ref, inv_ref, f_ref, e_ref, sems):
    copies = [pltpu.make_async_copy(e_hbm, e_ref, sems.at[0])]
    for g in range(4):
        part = pl.ds(4 * g, 4)
        copies.append(pltpu.make_async_copy(f_hbm.at[:, part], f_ref.at[:, part], sems.at[g + 1]))
    for copy in copies:
        copy.start()
    lane = lanes((CY, CZ))
    sums = {}

    def add(c, x, tile):
        g, s = z_slot(c, x)
        for side, keep in ((0, lane < GZ), (1, lane >= CZ - GZ)):
            part = roll(jnp.where(keep, tile, 0.0), GZ * (s + 1), 1)
            sums[g, side] = sums[g, side] + part if (g, side) in sums else part

    copies[0].wait()
    inv_ref[...] = 1.0 / e_ref[...]
    for x in range(CX):
        add(6, x, inv_ref[x])
    for g in range(4):
        copies[g + 1].wait()
        for x in range(4 * g, 4 * g + 4):
            for c in range(6):
                add(c, x, f_ref[c, x])
    for g in range(ZGROUPS):
        lo_ref[g] = sums[g, 0]
        hi_ref[g] = sums[g, 1]


def pack_y(f_ref, inv_ref, zlo_ref, zhi_ref, lo_ref, hi_ref):
    for out, start in ((lo_ref, 0), (hi_ref, 8)):
        rows = pl.ds(start, 8)
        for p in range(PAIRS):
            c, x = divmod(p, CX)
            out[p] = f_ref[c, x, rows] if c < 6 else inv_ref[x, rows]
        for g in range(ZGROUPS):
            out[PAIRS + g] = zlo_ref[g, rows]
            out[PAIRS + ZGROUPS + g] = zhi_ref[g, rows]


def z_ends(lo, hi, s, lane, t):
    first = lane < GZ * (s + 1) if s < 11 else (lane >= GZ * s) & (lane < GZ * (s + 1))
    moved = roll(jnp.where(first, lo, hi), 32 * t - GZ * s, 1)
    return jnp.where((lane >= 32 * t) & (lane < 32 * t + 2 * GZ), moved, 0.0)


def pack_x(f_ref, inv_ref, zlo_ref, zhi_ref, ylo_ref, yhi_ref, lo_ref, hi_ref):
    row = rows_of((8, CZ))

    def main_of(c, x, t):
        if t == 4:
            return jnp.where(row >= 4, main_of(c, x, 0), main_of(c, x, 3))
        if t in (1, 2):
            rows = pl.ds(8 * (t - 1), 8)
            return f_ref[c, x, rows] if c < 6 else inv_ref[x, rows]
        return (ylo_ref if t == 0 else yhi_ref)[c * CX + x]

    def end_of(g, t, e):
        if t == 4:
            return jnp.where(row >= 4, end_of(g, 0, e), end_of(g, 3, e))
        if t in (1, 2):
            return (zhi_ref if e else zlo_ref)[g, pl.ds(8 * (t - 1), 8)]
        return (ylo_ref if t == 0 else yhi_ref)[PAIRS + e * ZGROUPS + g]

    for out, side in ((lo_ref, 0), (hi_ref, 1)):
        for n, (k, c, t) in enumerate(XMAIN):
            out[n] = main_of(c, CX - k if side else k - 1, t)
        for (q, t, e), n in XEND.items():
            g = CX // 2 + side if q == 5 else (CX // 2 - 1 - q if side else q)
            out[n] = end_of(g, t, e)


def taylor(source, packed, inv_main, inv_packed, band, xs, tiles, scale, put, comps=(0, 1, 2, 3, 4, 5), skip=0):
    fields = [c for c in (4, 3, 1, 0) if {4: 0, 3: 1, 1: 3, 0: 4}[c] in comps]
    keys = [(i, c) for i in range(len(xs)) for c in fields]
    ghosts = three_parts(jnp.concatenate([packed[c, xs[i] - skip, pl.ds(8, 8)] for i, c in keys], axis=0))
    along_z = {}
    for t in tiles:
        mains = three_parts(jnp.concatenate([source[c, xs[i] - skip, band_of(t)] for i, c in keys], axis=0))
        left = [part for n in (2, 1, 0) for part in (mains[n], ghosts[n])]
        total = jnp.dot(jnp.concatenate(left, axis=1), jnp.concatenate([band[t]] * 3, axis=0), preferred_element_type=F32)
        for n, key in enumerate(keys):
            along_z[key + (t,)] = total[8 * n:8 * n + 8, 0:128]
            part = total[8 * n:8 * n + 8, 128:256]
            along_z[key + (4,)] = along_z[key + (4,)] + part if key + (4,) in along_z else part
    for i, x in enumerate(xs):
        for t in tuple(tiles) + (4,):
            one_tile(packed if t == 4 else source, inv_packed if t == 4 else inv_main, along_z, i, x, t, scale, put, comps, skip)


def one_tile(source, inv_ref, along_z, i, x, t, scale, put, comps, skip):
    def load(c, d=0, e=0):
        return source[c, x + d - skip, pl.ds(8 + e, 8) if t == 4 else band_of(t, e)]

    def dx(c):
        return load(c, 1) - load(c, -1), load(c, 2) - load(c, -2)

    def dy(c):
        return load(c, 0, 1) - load(c, 0, -1), load(c, 0, 2) - load(c, 0, -2)

    pairs = ((dy, 5, 4, 0), (None, 3, 5, dx), (dx, 4, 3, dy), (None, 1, 2, dy), (dx, 2, 0, 0), (dy, 0, 1, dx))
    inv = inv_ref[6, x, pl.ds(8, 8) if t == 4 else band_of(t)]
    factors = (inv * scale, jnp.where(inv > 0.0, scale, 0.0))
    for c in comps:
        first, c1, c2, second = pairs[c]
        if first and second:
            plus, minus = first(c1), second(c2)
            rate = 8.0 * (plus[0] - minus[0]) - (plus[1] - minus[1])
        elif first:
            plus = first(c1)
            rate = 8.0 * plus[0] - plus[1] - along_z[i, c2, t]
        else:
            minus = second(c2)
            rate = along_z[i, c1, t] - (8.0 * minus[0] - minus[1])
        put(c, x, t, factors[c // 3] * rate)


def store_packed(entries):
    for ref, c, x, value in entries:
        ref[c, x, pl.ds(8, 8)] = value
    for shift, start in ((32, 0), (-32, 16)):
        for ref, c, x, value in entries:
            if c in (0, 2, 3, 5):
                ref[c, x, pl.ds(start, 8)] = roll(value, shift, 1)


def packed_z(lane, t):
    place = lane - 32 * t
    inside = (place >= 0) & (place < 2 * GZ)
    return jnp.where(inside, jnp.where(place < GZ, place - GZ, place + (CZ - GZ)), -1000)


def dot(a, b, da=1, db=0):
    return lax.dot_general(a, b, (((da,), (db,)), ((), ())), precision=EXACT, preferred_element_type=F32)


def three_parts(value):
    high = value.astype(jnp.bfloat16)
    rest = value - high.astype(F32)
    middle = rest.astype(jnp.bfloat16)
    return high, middle, (rest - middle.astype(F32)).astype(jnp.bfloat16)


def split_dot(a, b):
    ah, am, _ = three_parts(a)
    bh, bm, _ = three_parts(b)
    return jnp.dot(
        jnp.concatenate([am, ah, ah], axis=1),
        jnp.concatenate([bh, bm, bh], axis=0),
        preferred_element_type=F32,
    )


def spread(count, parity):
    shape = (count, 128)
    return (lanes(shape) == rows_of(shape) + parity * 64).astype(F32)


def compute(
    f_ref, own_inv_ref, zlo_ref, zhi_ref, ylo_ref, yhi_ref, xlo_ref, xhi_ref, req_ref, band,
    new_ref, ans_ref,
    full, full_p, t1, t2, t3, p1, p2, p3, acc, acc_p, words, wz, wxy, spill, edge_rows, parts, sems,
):
    lane = lanes((8, CZ))
    row = rows_of((8, CZ))
    zero = jnp.zeros((8, CZ), F32)
    moves = []
    for p in range(PAIRS):
        c, x = divmod(p, CX)
        g, s = z_slot(c, x)
        for t in (0, 1, 2, 3):
            if t in (1, 2):
                own = pl.ds(8 * (t - 1), 8)
                full[c, GX + x, band_of(t)] = f_ref[c, x, own] if c < 6 else own_inv_ref[x, own]
                ends = (zlo_ref, (g, own)), (zhi_ref, (g, own))
            else:
                ref = ylo_ref if t == 0 else yhi_ref
                full[c, GX + x, band_of(t)] = ref[p]
                ends = (ref, PAIRS + g), (ref, PAIRS + ZGROUPS + g)
            moves.append((c, GX + x, t, s, ends, 0))
    for side in (0, 1):
        ref = xhi_ref if side == 0 else xlo_ref
        where_main = {key: n for n, key in enumerate(XMAIN)}
        for k in range(1, GX + 1):
            x = GX + CX + k - 1 if side == 0 else GX - k
            for c in range(NF):
                if k > 8 and c in (0, 3, 6):
                    continue
                g, s = z_slot(c, k - 1 if side == 0 else CX - k)
                q = 5 if c == 6 else (k - 1) // 2
                mains = [zero, zero, zero, zero]
                for t in (0, 1, 2, 3, 4):
                    if (k, c, t) in where_main:
                        value = ref[where_main[k, c, t]]
                        if t == 4:
                            mains[0], mains[3] = jnp.where(row >= 4, value, 0.0), jnp.where(row >= 4, 0.0, value)
                        else:
                            mains[t] = value
                    if (q, t, 0) in XEND:
                        ends = (ref, XEND[q, t, 0]), (ref, XEND[q, t, 1])
                        for u, part in ((0, 1), (3, 2)) if t == 4 else ((t, 0),):
                            moves.append((c, x, u, s, ends, part))
                for t in range(4):
                    full[c, x, band_of(t)] = mains[t]
    moves.sort(key=lambda m: ((32 * m[2] - GZ * m[3]) % 128, m[0], m[1]))
    begun = []
    for c, x, t, s, (low_end, high_end), part in moves:
        value = z_ends(low_end[0][low_end[1]], high_end[0][high_end[1]], s, lane, t)
        if part:
            value = jnp.where((row >= 4) if part == 1 else (row < 4), value, 0.0)
        if (c, x) in begun:
            value = value + full_p[c, x, pl.ds(8, 8)]
        else:
            begun.append((c, x))
        full_p[c, x, pl.ds(8, 8)] = value
    for shift, start in ((32, 0), (-32, 16)):
        for c, x in begun:
            if c in (0, 2, 3, 5):
                full_p[c, x, pl.ds(start, 8)] = roll(full_p[c, x, pl.ds(8, 8)], shift, 1)

    for power, source, packed, target, target_p in (
        (1, full, full_p, t1, p1), (2, t1, p1, t2, p2), (3, t2, p2, t3, p3)
    ):
        scale, skip = STEP / power / 12.0, 2 * power - 2

        waiting = []

        def put(c, x, t, value, target=target, target_p=target_p, power=power, waiting=waiting):
            if t == 4:
                waiting.append((target_p, c, x - 2 * power, value))
            else:
                target[c, x - 2 * power, band_of(t)] = value

        def body(i, carry, source=source, packed=packed, scale=scale, skip=skip, put=put, power=power, waiting=waiting):
            xs = [2 * power + 2 + ROWS * i + j for j in range(ROWS)]
            taylor(source, packed, full, full_p, band, xs, (0, 1, 2, 3), scale, put, skip=skip)
            store_packed(waiting)
            waiting.clear()
            return carry

        ends = [2 * power, 2 * power + 1, XW - 2 * power - 2, XW - 2 * power - 1]
        taylor(source, packed, full, full_p, band, ends, (1, 2), scale, put, (1, 2, 4, 5), skip)
        store_packed(waiting)
        waiting.clear()
        lax.fori_loop(0, (XW - 4 * power - 4) // ROWS, body, 0)

    def finish(c, x, t, value):
        if t == 4:
            terms = [ref[c, x - d, pl.ds(8, 8)] for ref, d in ((full_p, 0), (p1, 2), (p2, 4), (p3, 6))]
        else:
            terms = [ref[c, x - d, band_of(t)] for ref, d in ((full, 0), (t1, 2), (t2, 4), (t3, 6))]
        total = terms[0] + terms[1]
        total = total + terms[2]
        total = total + terms[3] + value
        if t == 4:
            acc_p[c, x - 8] = total
        else:
            acc[c, x - 8, t - 1] = total

    def last(i, carry):
        xs = [8 + ROWS * i + j for j in range(ROWS)]
        taylor(t3, p3, full, full_p, band, xs, (1, 2), STEP / 4 / 12.0, finish, skip=6)
        return carry

    lax.fori_loop(0, (XW - 16) // ROWS, last, 0)
    writes = [
        pltpu.make_async_copy(acc.at[:, pl.ds(2, CX), t], new_ref.at[:, :, pl.ds(8 * t, 8), :], sems.at[t])
        for t in (0, 1)
    ]
    for write in writes:
        write.start()

    req = req_ref[...]
    words[0] = dot(req, spread(64, 0), 0, 0)
    words[1] = dot(req, spread(64, 1), 0, 0)

    def word(pair, w):
        even = words[0, pl.ds(2 * pair * STRIDE + w, 1), :]
        return even + words[1, pl.ds((2 * pair + 1) * STRIDE + w, 1), :]

    cell = rows_of((CZ, 128)).astype(F32)
    low = rows_of((8, 128)).astype(F32)
    for pair in range(6):
        kind, at = divmod(pair, 2)
        columns = pl.ds(128 * at, 128)
        bx, by, bz = word(pair, 0), word(pair, 1), word(pair, 2)
        wx = [word(pair, 3 + i) for i in range(5)]
        wy = [word(pair, 8 + i) for i in range(5)]
        wz_rows = [word(pair, 13 + i) for i in range(5)]

        def weights(position, base, values):
            away = position - base
            total = jnp.zeros(away.shape, F32)
            for i in range(5):
                total = jnp.where(away == float(i), values[i], total)
            return total

        for t in ((1, 2), (2,), (1,))[kind]:
            use = (0, 1)[t - 1] if kind == 0 else kind + 1
            wz[use, pl.ds(0, CZ), columns] = weights(cell + 2.0, bz, wz_rows)
            ghost_z = packed_z(rows_of((CZ, 128)), t).astype(F32)
            wz[use, pl.ds(CZ, CZ), columns] = weights(ghost_z + 2.0, bz, wz_rows)
        in_x = [weights(jnp.full((1, 128), float(x), F32), bx, wx) for x in range(CX + 4)] if kind == 0 else []
        if kind == 0:
            for t in (0, 1):
                in_y = weights(low + (8.0 * t + 2.0), by, wy)
                for x in range(CX + 4):
                    wxy[x, t, :, columns] = in_x[x] * in_y
        else:
            pair_row = rows_of((8, 128))
            in_y = weights((pair_row % 2).astype(F32) + (16.0 if kind == 1 else 2.0), by, wy)
            for g in range(CX // 4 + 1):
                along = weights((pair_row // 2 + 4 * g).astype(F32), bx, wx)
                spill[kind - 1, g, :, columns] = along * in_y

    for kind in (0, 1):
        for half in (0, 1):
            for c in range(6):
                for g in range(CX // 4 + 1):
                    total = None
                    for i in range(4):
                        value = acc_p[c, 4 * g + i] if half else acc[c, 4 * g + i, 1 - kind]
                        moved = roll(value, 2 * i - (6 if kind == 0 else 0), 0)
                        total = moved if total is None else jnp.where(row >= 2 * i, moved, total)
                    edge_rows[kind, half, c, g] = total

    parts[...] = jnp.zeros((48, 128), F32)
    sums = {}
    for use in range(4):
        kind = max(use - 1, 0)
        if kind == 0:
            grid, weight = [acc[:, :, use], acc_p[...]], wxy[:, use].reshape(-1, 256)
        else:
            grid, weight = [edge_rows[kind - 1, half] for half in (0, 1)], spill[kind - 1].reshape(-1, 256)
        along = split_dot(jnp.concatenate([g.reshape(-1, CZ) for g in grid], axis=1), wz[use])
        count = weight.shape[0]
        for c in range(6):
            total = jnp.sum(along[c * count:c * count + count] * weight, axis=0, keepdims=True)
            sums[kind, c] = sums[kind, c] + total if (kind, c) in sums else total
    for (kind, c), total in sums.items():
        for at in (0, 1):
            parts[pl.ds((2 * kind + at) * 8 + c, 1), :] = total[:, 128 * at:128 * at + 128]
    values = parts[...]
    blank = jnp.zeros((16, 128), F32)
    filled = jnp.concatenate([values, blank], axis=0)
    empty = jnp.zeros((64, 128), F32)
    ans_ref[...] = dot(spread(64, 0), jnp.concatenate([filled, empty], axis=0), 1, 1) + dot(
        spread(64, 1), jnp.concatenate([empty, filled], axis=0), 1, 1
    )
    for write in writes:
        write.wait()


def requests(data_ref, send_ref, pick_ref, rank_ref, band_ref):
    for t in range(4):
        def places(index):
            return jnp.where(index < CZ, index, packed_z(index - CZ, t))

        apart = places(rows_of((256, 256))) - places(lanes((256, 256)))
        real = (places(rows_of((256, 256))) > -900) & (places(lanes((256, 256))) > -900)
        one = lambda d: ((apart == d) & real).astype(F32)
        stencil = (8.0 * (one(1) - one(-1)) + one(-2) - one(2)).astype(jnp.bfloat16)
        band_ref[t] = stencil

    data = data_ref[...]
    wide = (128, 128)
    owner = jnp.broadcast_to(data[:, 18:19], wide)
    base_y = jnp.broadcast_to(data[:, 1:2], wide)
    r, q = rows_of(wide), lanes(wide)
    owner_row = jnp.sum(jnp.where(r == q, owner, 0.0), axis=0, keepdims=True)
    base_row = jnp.sum(jnp.where(r == q, base_y, 0.0), axis=0, keepdims=True)
    same = owner == owner_row
    rank_col = jnp.sum(jnp.where(same & (q < r), 1.0, 0.0), axis=1, keepdims=True)
    rank_row = jnp.sum(jnp.where(same & (r < q), 1.0, 0.0), axis=0, keepdims=True)
    rank_ref[...] = jnp.broadcast_to(rank_row, (8, 128))

    lane = lanes((128, 256))
    slot, w = lane // STRIDE, lane % STRIDE
    word_row = rows_of((128, 256))
    copies = jnp.where((lanes((128, 256)) % STRIDE == word_row) & (word_row < 18) & (lane < 12 * STRIDE), 1.0, 0.0)
    spread_out = dot(data, copies)
    moved = jnp.where(w == 1, jnp.where(slot // 4 == 1, float(CY), jnp.where(slot // 4 == 2, -float(CY), 0.0)), 0.0)
    chosen = (slot % 4).astype(F32) == rank_col
    spread_out = jnp.where(chosen, spread_out + moved, 0.0)

    place = rows_of((64, 128)).astype(F32)
    total = jnp.zeros((64, 256), F32)
    for kind, move in ((0, 0.0), (1, -16.0), (2, 16.0)):
        hit = place == owner_row + move
        if kind == 1:
            hit = hit & (base_row < 2.0)
        if kind == 2:
            hit = hit & (base_row > 13.0)
        pick = jnp.where(hit, 1.0, 0.0)
        pick_ref[kind] = pick
        total = total + dot(pick, jnp.where(slot // 4 == kind, spread_out, 0.0))
    send_ref[...] = total


def collect(ans_ref, pick_ref, rank_ref, out_ref):
    ans = ans_ref[...]
    rank = rank_ref[...]
    total = jnp.zeros((8, 128), F32)
    for kind in range(3):
        got = dot(ans, pick_ref[kind], 0, 0)
        for j in range(4):
            start = (j % 2) * 64 + (2 * kind + j // 2) * 8
            total = total + jnp.where(rank == float(j), got[start:start + 8], 0.0)
    out_ref[...] = total[0:6]


def shift_both(low_edge, high_edge, axis):
    size = lax.axis_size(axis)
    up = [(i, i + 1) for i in range(size - 1)]
    down = [(i + 1, i) for i in range(size - 1)]
    return lax.ppermute(high_edge, axis, up), lax.ppermute(low_edge, axis, down)


def local(fields, permittivity, donor_owner, donor_base, donor_weights):
    data = jnp.concatenate(
        [
            donor_base.astype(F32),
            donor_weights,
            donor_owner.astype(F32),
            jnp.zeros((donor_owner.shape[0], 128 - 19), F32),
        ],
        axis=1,
    )
    zshape = (ZGROUPS, CY, CZ)
    zlo, zhi, inv = call(
        pack_z,
        [zshape, zshape, (CX, CY, CZ)],
        (fields, permittivity),
        53,
        scratch=[
            pltpu.VMEM((6, CX, CY, CZ), F32),
            pltpu.VMEM((CX, CY, CZ), F32),
            pltpu.SemaphoreType.DMA((5,)),
        ],
        space=pltpu.HBM,
    )
    zlo, zhi = shift_both(zlo, zhi, "gz")
    yshape = (YTOTAL, 8, CZ)
    ylo, yhi = call(pack_y, [yshape, yshape], (fields, inv, zlo, zhi), 8)
    ylo, yhi = shift_both(ylo, yhi, "gy")
    xshape = (XTOTAL, 8, CZ)
    xlo, xhi = call(pack_x, [xshape, xshape], (fields, inv, zlo, zhi, ylo, yhi), 8)
    send, pick, rank, band = call(requests, [(64, 256), (3, 64, 128), (8, 128), (4, 256, 256)], (data,), 8)
    send, xlo, xhi = lax.optimization_barrier((send, xlo, xhi))
    xlo, xhi = shift_both(xlo, xhi, "gx")
    req = lax.all_to_all(send, ("gy", "gz"), 0, 0, tiled=True)
    new_fields, answers = call(
        compute,
        [(6, CX, CY, CZ), (64, 128)],
        (fields, inv, zlo, zhi, ylo, yhi, xlo, xhi, req, band),
        40,
        scratch=[
            pltpu.VMEM((NF, XW, 48, CZ), F32),
            pltpu.VMEM((NF, XW, 24, CZ), F32),
            *[pltpu.VMEM((6, XW - 4 * m, 48, CZ), F32) for m in (1, 2, 3)],
            *[pltpu.VMEM((6, XW - 4 * m, 24, CZ), F32) for m in (1, 2, 3)],
            pltpu.VMEM((6, CX + 4, 2, 8, CZ), F32),
            pltpu.VMEM((6, CX + 4, 8, CZ), F32),
            pltpu.VMEM((2, 256, 128), F32),
            pltpu.VMEM((4, 256, 256), F32),
            pltpu.VMEM((CX + 4, 2, 8, 256), F32),
            pltpu.VMEM((2, CX // 4 + 1, 8, 256), F32),
            pltpu.VMEM((2, 2, 6, CX // 4 + 1, 8, CZ), F32),
            pltpu.VMEM((48, 128), F32),
            pltpu.SemaphoreType.DMA((2,)),
        ],
        flops=100000000,
        first=pl.ANY,
    )
    answers = lax.all_to_all(answers, ("gy", "gz"), 0, 0, tiled=True)
    receptor_values = call(collect, (6, 128), (answers, pick, rank), 8)
    return new_fields, receptor_values


def solution(mesh):
    placed = (
        P(None, "gx", "gy", "gz"),
        P("gx", "gy", "gz"),
        P(("gx", "gy", "gz"), None),
        P(("gx", "gy", "gz"), None),
        P(("gx", "gy", "gz"), None),
    )
    return jax.shard_map(
        local,
        mesh=mesh,
        in_specs=placed,
        out_specs=(P(None, "gx", "gy", "gz"), P(None, ("gx", "gy", "gz"))),
        check_vma=False,
    )
```

```python
import jax
import jax.numpy as jnp
from jax import lax
from jax.experimental import pallas as pl
from jax.experimental.pallas import tpu as pltpu
from jax.sharding import PartitionSpec as P

STEP = 0.25
CX, CY, CZ = 16, 16, 128
GX, GZ = 10, 10
NF = 7
PAIRS = NF * CX
ZGROUPS = CX // 2 + 2
XW = CX + 2 * GX
STRIDE = 20
ROWS = 4
EXACT = lax.Precision.HIGHEST
F32 = jnp.float32


def band_of(t, d=0):
    return pl.ds(8 + 8 * t + d, 8)


def z_slot(c, x):
    return (x // 2, (x % 2) * 6 + c) if c < 6 else (CX // 2 + x // 8, x % 8)


def x_lists():
    main = []
    for k in range(1, 5):
        main += [(k, c, t) for c in range(NF) for t in (0, 1, 2, 3)]
    for k in range(5, 7):
        main += [(k, c, t) for c in range(NF) for t in (1, 2, 4)]
    for k in range(7, 9):
        main += [(k, c, t) for c in range(NF) for t in (1, 2)]
        main += [(k, c, 4) for c in (0, 3)]
    for k in range(9, 11):
        main += [(k, c, t) for c in (1, 2, 4, 5) for t in (1, 2)]
    ends = []
    for q in range(5):
        ends += [(q, t, e) for t in ((0, 1, 2, 3), (0, 1, 2, 3), (1, 2, 4), (1, 2, 4), (1, 2))[q] for e in (0, 1)]
    ends += [(5, t, e) for t in (0, 1, 2, 3) for e in (0, 1)]
    return main, ends


XMAIN, XENDS = x_lists()
XROWS = len(XMAIN)
XEND = {key: XROWS + n for n, key in enumerate(XENDS)}
XTOTAL = XROWS + len(XENDS)
YTOTAL = PAIRS + 2 * ZGROUPS


def roll(value, shift, axis):
    size = value.shape[axis]
    shift = shift % size
    return value if shift == 0 else pltpu.roll(value, shift, axis)


def lanes(shape):
    return lax.broadcasted_iota(jnp.int32, shape, len(shape) - 1)


def rows_of(shape):
    return lax.broadcasted_iota(jnp.int32, shape, len(shape) - 2)


def vmem(count):
    return [pl.BlockSpec(memory_space=pltpu.VMEM)] * count


def call(body, outs, ins, limit, scratch=(), flops=1000000, space=pltpu.VMEM, first=pltpu.VMEM):
    many = isinstance(outs, list)
    return pl.pallas_call(
        body,
        out_shape=[jax.ShapeDtypeStruct(s, jnp.bfloat16 if s == (4, 256, 256) else F32) for s in outs]
        if many
        else jax.ShapeDtypeStruct(outs, F32),
        in_specs=[pl.BlockSpec(memory_space=space)] * len(ins),
        out_specs=[pl.BlockSpec(memory_space=first)] + vmem(len(outs) - 1) if many else vmem(1)[0],
        scratch_shapes=list(scratch),
        compiler_params=pltpu.CompilerParams(vmem_limit_bytes=limit * 1048576),
        cost_estimate=pl.CostEstimate(flops=flops, bytes_accessed=1000000, transcendentals=0),
    )(*ins)


def pack_z(f_hbm, e_hbm, lo_ref, hi_ref, inv_ref, f_ref, e_ref, sems):
    copies = [pltpu.make_async_copy(e_hbm, e_ref, sems.at[0])]
    for g in range(4):
        part = pl.ds(4 * g, 4)
        copies.append(pltpu.make_async_copy(f_hbm.at[:, part], f_ref.at[:, part], sems.at[g + 1]))
    for copy in copies:
        copy.start()
    lane = lanes((CY, CZ))
    sums = {}

    def add(c, x, tile):
        g, s = z_slot(c, x)
        for side, keep in ((0, lane < GZ), (1, lane >= CZ - GZ)):
            part = roll(jnp.where(keep, tile, 0.0), GZ * (s + 1), 1)
            sums[g, side] = sums[g, side] + part if (g, side) in sums else part

    copies[0].wait()
    inv_ref[...] = 1.0 / e_ref[...]
    for x in range(CX):
        add(6, x, inv_ref[x])
    for g in range(4):
        copies[g + 1].wait()
        for x in range(4 * g, 4 * g + 4):
            for c in range(6):
                add(c, x, f_ref[c, x])
    for g in range(ZGROUPS):
        lo_ref[g] = sums[g, 0]
        hi_ref[g] = sums[g, 1]


def pack_y(f_ref, inv_ref, zlo_ref, zhi_ref, lo_ref, hi_ref):
    for out, start in ((lo_ref, 0), (hi_ref, 8)):
        rows = pl.ds(start, 8)
        for p in range(PAIRS):
            c, x = divmod(p, CX)
            out[p] = f_ref[c, x, rows] if c < 6 else inv_ref[x, rows]
        for g in range(ZGROUPS):
            out[PAIRS + g] = zlo_ref[g, rows]
            out[PAIRS + ZGROUPS + g] = zhi_ref[g, rows]


def z_ends(lo, hi, s, lane, t):
    first = lane < GZ * (s + 1) if s < 11 else (lane >= GZ * s) & (lane < GZ * (s + 1))
    moved = roll(jnp.where(first, lo, hi), 32 * t - GZ * s, 1)
    return jnp.where((lane >= 32 * t) & (lane < 32 * t + 2 * GZ), moved, 0.0)


def pack_x(f_ref, inv_ref, zlo_ref, zhi_ref, ylo_ref, yhi_ref, lo_ref, hi_ref):
    row = rows_of((8, CZ))

    def main_of(c, x, t):
        if t == 4:
            return jnp.where(row >= 4, main_of(c, x, 0), main_of(c, x, 3))
        if t in (1, 2):
            rows = pl.ds(8 * (t - 1), 8)
            return f_ref[c, x, rows] if c < 6 else inv_ref[x, rows]
        return (ylo_ref if t == 0 else yhi_ref)[c * CX + x]

    def end_of(g, t, e):
        if t == 4:
            return jnp.where(row >= 4, end_of(g, 0, e), end_of(g, 3, e))
        if t in (1, 2):
            return (zhi_ref if e else zlo_ref)[g, pl.ds(8 * (t - 1), 8)]
        return (ylo_ref if t == 0 else yhi_ref)[PAIRS + e * ZGROUPS + g]

    for out, side in ((lo_ref, 0), (hi_ref, 1)):
        for n, (k, c, t) in enumerate(XMAIN):
            out[n] = main_of(c, CX - k if side else k - 1, t)
        for (q, t, e), n in XEND.items():
            g = CX // 2 + side if q == 5 else (CX // 2 - 1 - q if side else q)
            out[n] = end_of(g, t, e)


def taylor(source, packed, inv_main, inv_packed, band, xs, tiles, scale, put, comps=(0, 1, 2, 3, 4, 5), skip=0, flush=None):
    fields = [c for c in (4, 3, 1, 0) if {4: 0, 3: 1, 1: 3, 0: 4}[c] in comps]
    keys = [(i, c) for i in range(len(xs)) for c in fields]
    ghosts = three_parts(jnp.concatenate([packed[c, xs[i] - skip, pl.ds(8, 8)] for i, c in keys], axis=0))
    along_z = {}
    for t in tiles:
        mains = three_parts(jnp.concatenate([source[c, xs[i] - skip, band_of(t)] for i, c in keys], axis=0))
        left = [part for n in (2, 1, 0) for part in (mains[n], ghosts[n])]
        total = jnp.dot(jnp.concatenate(left, axis=1), jnp.concatenate([band[t]] * 3, axis=0), preferred_element_type=F32)
        for n, key in enumerate(keys):
            along_z[key + (t,)] = total[8 * n:8 * n + 8, 0:128]
            part = total[8 * n:8 * n + 8, 128:256]
            along_z[key + (4,)] = along_z[key + (4,)] + part if key + (4,) in along_z else part
    for i, x in enumerate(xs):
        one_tile(packed, inv_packed, along_z, i, x, 4, scale, put, comps, skip)
    if flush:
        flush()
    for i, x in enumerate(xs):
        for t in tiles:
            one_tile(source, inv_main, along_z, i, x, t, scale, put, comps, skip)


def one_tile(source, inv_ref, along_z, i, x, t, scale, put, comps, skip):
    def load(c, d=0, e=0):
        return source[c, x + d - skip, pl.ds(8 + e, 8) if t == 4 else band_of(t, e)]

    def dx(c):
        return load(c, 1) - load(c, -1), load(c, 2) - load(c, -2)

    def dy(c):
        return load(c, 0, 1) - load(c, 0, -1), load(c, 0, 2) - load(c, 0, -2)

    pairs = ((dy, 5, 4, 0), (None, 3, 5, dx), (dx, 4, 3, dy), (None, 1, 2, dy), (dx, 2, 0, 0), (dy, 0, 1, dx))
    inv = inv_ref[6, x, pl.ds(8, 8) if t == 4 else band_of(t)]
    factors = (inv * scale, jnp.where(inv > 0.0, scale, 0.0))
    for c in comps:
        first, c1, c2, second = pairs[c]
        if first and second:
            plus, minus = first(c1), second(c2)
            rate = 8.0 * (plus[0] - minus[0]) - (plus[1] - minus[1])
        elif first:
            plus = first(c1)
            rate = 8.0 * plus[0] - plus[1] - along_z[i, c2, t]
        else:
            minus = second(c2)
            rate = along_z[i, c1, t] - (8.0 * minus[0] - minus[1])
        put(c, x, t, factors[c // 3] * rate)


def store_packed(entries):
    for ref, c, x, value in entries:
        ref[c, x, pl.ds(8, 8)] = value
    for shift, start in ((32, 0), (-32, 16)):
        for ref, c, x, value in entries:
            if c in (0, 2, 3, 5):
                ref[c, x, pl.ds(start, 8)] = roll(value, shift, 1)


def packed_z(lane, t):
    place = lane - 32 * t
    inside = (place >= 0) & (place < 2 * GZ)
    return jnp.where(inside, jnp.where(place < GZ, place - GZ, place + (CZ - GZ)), -1000)


def dot(a, b, da=1, db=0):
    return lax.dot_general(a, b, (((da,), (db,)), ((), ())), precision=EXACT, preferred_element_type=F32)


def three_parts(value):
    high = value.astype(jnp.bfloat16)
    rest = value - high.astype(F32)
    middle = rest.astype(jnp.bfloat16)
    return high, middle, (rest - middle.astype(F32)).astype(jnp.bfloat16)


def split_dot(a, b):
    ah, am, _ = three_parts(a)
    bh, bm, _ = three_parts(b)
    return jnp.dot(
        jnp.concatenate([am, ah, ah], axis=1),
        jnp.concatenate([bh, bm, bh], axis=0),
        preferred_element_type=F32,
    )


def spread(count, parity):
    shape = (count, 128)
    return (lanes(shape) == rows_of(shape) + parity * 64).astype(F32)


def compute(
    f_ref, own_inv_ref, zlo_ref, zhi_ref, ylo_ref, yhi_ref, xlo_ref, xhi_ref, req_ref, band,
    new_ref, ans_ref,
    full, full_p, t1, t2, t3, p1, p2, p3, acc, acc_p, words, wz, wxy, spill, edge_rows, parts, sems,
):
    lane = lanes((8, CZ))
    row = rows_of((8, CZ))
    zero = jnp.zeros((8, CZ), F32)
    moves = []
    for p in range(PAIRS):
        c, x = divmod(p, CX)
        g, s = z_slot(c, x)
        for t in (0, 1, 2, 3):
            if t in (1, 2):
                own = pl.ds(8 * (t - 1), 8)
                full[c, GX + x, band_of(t)] = f_ref[c, x, own] if c < 6 else own_inv_ref[x, own]
                ends = (zlo_ref, (g, own)), (zhi_ref, (g, own))
            else:
                ref = ylo_ref if t == 0 else yhi_ref
                full[c, GX + x, band_of(t)] = ref[p]
                ends = (ref, PAIRS + g), (ref, PAIRS + ZGROUPS + g)
            moves.append((c, GX + x, t, s, ends, 0))
    for side in (0, 1):
        ref = xhi_ref if side == 0 else xlo_ref
        where_main = {key: n for n, key in enumerate(XMAIN)}
        for k in range(1, GX + 1):
            x = GX + CX + k - 1 if side == 0 else GX - k
            for c in range(NF):
                if k > 8 and c in (0, 3, 6):
                    continue
                g, s = z_slot(c, k - 1 if side == 0 else CX - k)
                q = 5 if c == 6 else (k - 1) // 2
                mains = [zero, zero, zero, zero]
                for t in (0, 1, 2, 3, 4):
                    if (k, c, t) in where_main:
                        value = ref[where_main[k, c, t]]
                        if t == 4:
                            mains[0], mains[3] = jnp.where(row >= 4, value, 0.0), jnp.where(row >= 4, 0.0, value)
                        else:
                            mains[t] = value
                    if (q, t, 0) in XEND:
                        ends = (ref, XEND[q, t, 0]), (ref, XEND[q, t, 1])
                        for u, part in ((0, 1), (3, 2)) if t == 4 else ((t, 0),):
                            moves.append((c, x, u, s, ends, part))
                for t in range(4):
                    full[c, x, band_of(t)] = mains[t]
    moves.sort(key=lambda m: ((32 * m[2] - GZ * m[3]) % 128, m[0], m[1]))
    begun = []
    for c, x, t, s, (low_end, high_end), part in moves:
        value = z_ends(low_end[0][low_end[1]], high_end[0][high_end[1]], s, lane, t)
        if part:
            value = jnp.where((row >= 4) if part == 1 else (row < 4), value, 0.0)
        if (c, x) in begun:
            value = value + full_p[c, x, pl.ds(8, 8)]
        else:
            begun.append((c, x))
        full_p[c, x, pl.ds(8, 8)] = value
    for shift, start in ((32, 0), (-32, 16)):
        for c, x in begun:
            if c in (0, 2, 3, 5):
                full_p[c, x, pl.ds(start, 8)] = roll(full_p[c, x, pl.ds(8, 8)], shift, 1)

    for power, source, packed, target, target_p in (
        (1, full, full_p, t1, p1), (2, t1, p1, t2, p2), (3, t2, p2, t3, p3)
    ):
        scale, skip = STEP / power / 12.0, 2 * power - 2

        waiting = []

        def flush(waiting=waiting):
            store_packed(waiting)
            waiting.clear()

        def put(c, x, t, value, target=target, target_p=target_p, power=power, waiting=waiting):
            if t == 4:
                waiting.append((target_p, c, x - 2 * power, value))
            else:
                target[c, x - 2 * power, band_of(t)] = value

        def body(i, carry, source=source, packed=packed, scale=scale, skip=skip, put=put, power=power, flush=flush):
            xs = [2 * power + 2 + ROWS * i + j for j in range(ROWS)]
            taylor(source, packed, full, full_p, band, xs, (0, 1, 2, 3), scale, put, skip=skip, flush=flush)
            return carry

        ends = [2 * power, 2 * power + 1, XW - 2 * power - 2, XW - 2 * power - 1]
        taylor(source, packed, full, full_p, band, ends, (1, 2), scale, put, (1, 2, 4, 5), skip, flush)
        lax.fori_loop(0, (XW - 4 * power - 4) // ROWS, body, 0)

    def finish(c, x, t, value):
        if t == 4:
            terms = [ref[c, x - d, pl.ds(8, 8)] for ref, d in ((full_p, 0), (p1, 2), (p2, 4), (p3, 6))]
        else:
            terms = [ref[c, x - d, band_of(t)] for ref, d in ((full, 0), (t1, 2), (t2, 4), (t3, 6))]
        total = terms[0] + terms[1]
        total = total + terms[2]
        total = total + terms[3] + value
        if t == 4:
            acc_p[c, x - 8] = total
        else:
            acc[c, x - 8, t - 1] = total

    def last(i, carry):
        xs = [8 + ROWS * i + j for j in range(ROWS)]
        taylor(t3, p3, full, full_p, band, xs, (1, 2), STEP / 4 / 12.0, finish, skip=6)
        return carry

    lax.fori_loop(0, (XW - 16) // ROWS, last, 0)
    writes = [
        pltpu.make_async_copy(acc.at[:, pl.ds(2, CX), t], new_ref.at[:, :, pl.ds(8 * t, 8), :], sems.at[t])
        for t in (0, 1)
    ]
    for write in writes:
        write.start()

    req = req_ref[...]
    words[0] = dot(req, spread(64, 0), 0, 0)
    words[1] = dot(req, spread(64, 1), 0, 0)

    def word(pair, w):
        even = words[0, pl.ds(2 * pair * STRIDE + w, 1), :]
        return even + words[1, pl.ds((2 * pair + 1) * STRIDE + w, 1), :]

    cell = rows_of((CZ, 128)).astype(F32)
    low = rows_of((8, 128)).astype(F32)
    for pair in range(6):
        kind, at = divmod(pair, 2)
        columns = pl.ds(128 * at, 128)
        bx, by, bz = word(pair, 0), word(pair, 1), word(pair, 2)
        wx = [word(pair, 3 + i) for i in range(5)]
        wy = [word(pair, 8 + i) for i in range(5)]
        wz_rows = [word(pair, 13 + i) for i in range(5)]

        def weights(position, base, values):
            away = position - base
            total = jnp.zeros(away.shape, F32)
            for i in range(5):
                total = jnp.where(away == float(i), values[i], total)
            return total

        for t in ((1, 2), (2,), (1,))[kind]:
            use = (0, 1)[t - 1] if kind == 0 else kind + 1
            wz[use, pl.ds(0, CZ), columns] = weights(cell + 2.0, bz, wz_rows)
            ghost_z = packed_z(rows_of((CZ, 128)), t).astype(F32)
            wz[use, pl.ds(CZ, CZ), columns] = weights(ghost_z + 2.0, bz, wz_rows)
        in_x = [weights(jnp.full((1, 128), float(x), F32), bx, wx) for x in range(CX + 4)] if kind == 0 else []
        if kind == 0:
            for t in (0, 1):
                in_y = weights(low + (8.0 * t + 2.0), by, wy)
                for x in range(CX + 4):
                    wxy[x, t, :, columns] = in_x[x] * in_y
        else:
            pair_row = rows_of((8, 128))
            in_y = weights((pair_row % 2).astype(F32) + (16.0 if kind == 1 else 2.0), by, wy)
            for g in range(CX // 4 + 1):
                along = weights((pair_row // 2 + 4 * g).astype(F32), bx, wx)
                spill[kind - 1, g, :, columns] = along * in_y

    for kind in (0, 1):
        for half in (0, 1):
            for c in range(6):
                for g in range(CX // 4 + 1):
                    total = None
                    for i in range(4):
                        value = acc_p[c, 4 * g + i] if half else acc[c, 4 * g + i, 1 - kind]
                        moved = roll(value, 2 * i - (6 if kind == 0 else 0), 0)
                        total = moved if total is None else jnp.where(row >= 2 * i, moved, total)
                    edge_rows[kind, half, c, g] = total

    parts[...] = jnp.zeros((48, 128), F32)
    sums = {}
    for use in range(4):
        kind = max(use - 1, 0)
        if kind == 0:
            grid, weight = [acc[:, :, use], acc_p[...]], wxy[:, use].reshape(-1, 256)
        else:
            grid, weight = [edge_rows[kind - 1, half] for half in (0, 1)], spill[kind - 1].reshape(-1, 256)
        along = split_dot(jnp.concatenate([g.reshape(-1, CZ) for g in grid], axis=1), wz[use])
        count = weight.shape[0]
        for c in range(6):
            total = jnp.sum(along[c * count:c * count + count] * weight, axis=0, keepdims=True)
            sums[kind, c] = sums[kind, c] + total if (kind, c) in sums else total
    for (kind, c), total in sums.items():
        for at in (0, 1):
            parts[pl.ds((2 * kind + at) * 8 + c, 1), :] = total[:, 128 * at:128 * at + 128]
    values = parts[...]
    blank = jnp.zeros((16, 128), F32)
    filled = jnp.concatenate([values, blank], axis=0)
    empty = jnp.zeros((64, 128), F32)
    ans_ref[...] = dot(spread(64, 0), jnp.concatenate([filled, empty], axis=0), 1, 1) + dot(
        spread(64, 1), jnp.concatenate([empty, filled], axis=0), 1, 1
    )
    for write in writes:
        write.wait()


def requests(data_ref, send_ref, pick_ref, rank_ref, band_ref):
    for t in range(4):
        def places(index):
            return jnp.where(index < CZ, index, packed_z(index - CZ, t))

        apart = places(rows_of((256, 256))) - places(lanes((256, 256)))
        real = (places(rows_of((256, 256))) > -900) & (places(lanes((256, 256))) > -900)
        one = lambda d: ((apart == d) & real).astype(F32)
        stencil = (8.0 * (one(1) - one(-1)) + one(-2) - one(2)).astype(jnp.bfloat16)
        band_ref[t] = stencil

    data = data_ref[...]
    wide = (128, 128)
    owner = jnp.broadcast_to(data[:, 18:19], wide)
    base_y = jnp.broadcast_to(data[:, 1:2], wide)
    r, q = rows_of(wide), lanes(wide)
    owner_row = jnp.sum(jnp.where(r == q, owner, 0.0), axis=0, keepdims=True)
    base_row = jnp.sum(jnp.where(r == q, base_y, 0.0), axis=0, keepdims=True)
    same = owner == owner_row
    rank_col = jnp.sum(jnp.where(same & (q < r), 1.0, 0.0), axis=1, keepdims=True)
    rank_row = jnp.sum(jnp.where(same & (r < q), 1.0, 0.0), axis=0, keepdims=True)
    rank_ref[...] = jnp.broadcast_to(rank_row, (8, 128))

    lane = lanes((128, 256))
    slot, w = lane // STRIDE, lane % STRIDE
    word_row = rows_of((128, 256))
    copies = jnp.where((lanes((128, 256)) % STRIDE == word_row) & (word_row < 18) & (lane < 12 * STRIDE), 1.0, 0.0)
    spread_out = dot(data, copies)
    moved = jnp.where(w == 1, jnp.where(slot // 4 == 1, float(CY), jnp.where(slot // 4 == 2, -float(CY), 0.0)), 0.0)
    chosen = (slot % 4).astype(F32) == rank_col
    spread_out = jnp.where(chosen, spread_out + moved, 0.0)

    place = rows_of((64, 128)).astype(F32)
    total = jnp.zeros((64, 256), F32)
    for kind, move in ((0, 0.0), (1, -16.0), (2, 16.0)):
        hit = place == owner_row + move
        if kind == 1:
            hit = hit & (base_row < 2.0)
        if kind == 2:
            hit = hit & (base_row > 13.0)
        pick = jnp.where(hit, 1.0, 0.0)
        pick_ref[kind] = pick
        total = total + dot(pick, jnp.where(slot // 4 == kind, spread_out, 0.0))
    send_ref[...] = total


def collect(ans_ref, pick_ref, rank_ref, out_ref):
    ans = ans_ref[...]
    rank = rank_ref[...]
    total = jnp.zeros((8, 128), F32)
    for kind in range(3):
        got = dot(ans, pick_ref[kind], 0, 0)
        for j in range(4):
            start = (j % 2) * 64 + (2 * kind + j // 2) * 8
            total = total + jnp.where(rank == float(j), got[start:start + 8], 0.0)
    out_ref[...] = total[0:6]


def shift_both(low_edge, high_edge, axis):
    size = lax.axis_size(axis)
    up = [(i, i + 1) for i in range(size - 1)]
    down = [(i + 1, i) for i in range(size - 1)]
    return lax.ppermute(high_edge, axis, up), lax.ppermute(low_edge, axis, down)


def local(fields, permittivity, donor_owner, donor_base, donor_weights):
    data = jnp.concatenate(
        [
            donor_base.astype(F32),
            donor_weights,
            donor_owner.astype(F32),
            jnp.zeros((donor_owner.shape[0], 128 - 19), F32),
        ],
        axis=1,
    )
    zshape = (ZGROUPS, CY, CZ)
    zlo, zhi, inv = call(
        pack_z,
        [zshape, zshape, (CX, CY, CZ)],
        (fields, permittivity),
        53,
        scratch=[
            pltpu.VMEM((6, CX, CY, CZ), F32),
            pltpu.VMEM((CX, CY, CZ), F32),
            pltpu.SemaphoreType.DMA((5,)),
        ],
        space=pltpu.HBM,
    )
    zlo, zhi = shift_both(zlo, zhi, "gz")
    yshape = (YTOTAL, 8, CZ)
    ylo, yhi = call(pack_y, [yshape, yshape], (fields, inv, zlo, zhi), 8)
    ylo, yhi = shift_both(ylo, yhi, "gy")
    xshape = (XTOTAL, 8, CZ)
    xlo, xhi = call(pack_x, [xshape, xshape], (fields, inv, zlo, zhi, ylo, yhi), 8)
    send, pick, rank, band = call(requests, [(64, 256), (3, 64, 128), (8, 128), (4, 256, 256)], (data,), 8)
    send, xlo, xhi = lax.optimization_barrier((send, xlo, xhi))
    xlo, xhi = shift_both(xlo, xhi, "gx")
    req = lax.all_to_all(send, ("gy", "gz"), 0, 0, tiled=True)
    new_fields, answers = call(
        compute,
        [(6, CX, CY, CZ), (64, 128)],
        (fields, inv, zlo, zhi, ylo, yhi, xlo, xhi, req, band),
        40,
        scratch=[
            pltpu.VMEM((NF, XW, 48, CZ), F32),
            pltpu.VMEM((NF, XW, 24, CZ), F32),
            *[pltpu.VMEM((6, XW - 4 * m, 48, CZ), F32) for m in (1, 2, 3)],
            *[pltpu.VMEM((6, XW - 4 * m, 24, CZ), F32) for m in (1, 2, 3)],
            pltpu.VMEM((6, CX + 4, 2, 8, CZ), F32),
            pltpu.VMEM((6, CX + 4, 8, CZ), F32),
            pltpu.VMEM((2, 256, 128), F32),
            pltpu.VMEM((4, 256, 256), F32),
            pltpu.VMEM((CX + 4, 2, 8, 256), F32),
            pltpu.VMEM((2, CX // 4 + 1, 8, 256), F32),
            pltpu.VMEM((2, 2, 6, CX // 4 + 1, 8, CZ), F32),
            pltpu.VMEM((48, 128), F32),
            pltpu.SemaphoreType.DMA((2,)),
        ],
        flops=100000000,
        first=pl.ANY,
    )
    answers = lax.all_to_all(answers, ("gy", "gz"), 0, 0, tiled=True)
    receptor_values = call(collect, (6, 128), (answers, pick, rank), 8)
    return new_fields, receptor_values


def solution(mesh):
    placed = (
        P(None, "gx", "gy", "gz"),
        P("gx", "gy", "gz"),
        P(("gx", "gy", "gz"), None),
        P(("gx", "gy", "gz"), None),
        P(("gx", "gy", "gz"), None),
    )
    return jax.shard_map(
        local,
        mesh=mesh,
        in_specs=placed,
        out_specs=(P(None, "gx", "gy", "gz"), P(None, ("gx", "gy", "gz"))),
        check_vma=False,
    )
```
